256 devices in a mesh: gx: 8 (over z_hi, core), gz: 32 (over x, z_lo, y).
Axes of the slice: x: 4, y: 4, z: 8 (z_hi: 4, z_lo: 2; z = z_hi * 2 + z_lo), core: 2. Of those that a mesh axis runs over, the one named last changes fastest.
Arguments:
- modes: bfloat16 [3, 16, 128, 256, 128], P(None, 'gx', None, 'gz'), may hold values from -6 to 6
- weights: float32 [16, 128, 256], P('gx', None, 'gz'), may hold values from 0.0007973615 to 0.007973615
- counts: int32 [256], P(('gx', 'gz')), may hold values from 1 to 128, 10922 in all
- mode_index: int32 [16], replicated, may hold values from 0 to 127, as said below
Outputs:
- slices: float32 [16, 128, 128], P(None, 'gz')
The draws below stay inside these ranges and needn't reach their ends.
Inputs may be any that keep to these rules, and one draw needn't show every extreme that they name: `mode_index`: distinct modes. The counts sum to 128 * 8 * 32 // 3 and one pencil holds 128.
All inputs are finite; a program needn't handle non-finite values. No bound on the sum of `counts` on one device may be relied on, other than what follows from the above.
Results may differ from the reference program's by a relative error of at most 0.004.
Values may be sent and summed in bfloat16 or wider, within the bound.
A program may use at most 64 MiB of HBM per device.

```python
import math
import jax
import jax.numpy as jnp
import numpy as np
from jax import lax

M = 128
JW = 16
CX = 2
CZ = 8
YCAP = 128
NX = 16
NZ = 256
N_GX = 8
N_GZ = 32
DEVICES = 256


def draw_mode_index(key, part):
    return jax.random.permutation(key, M)[:JW].astype(jnp.int32)


def block_levels(stream_key, extent, cuts, least, top_value):
    gain = 1.0
    for dim, parts in cuts:
        heights = jax.random.uniform(jax.random.fold_in(jax.random.fold_in(stream_key, 6), dim), (parts,), jnp.float32, least / len(cuts), top_value / len(cuts))
        gain = gain * jnp.repeat(jnp.exp(heights), extent[dim] // parts).reshape((-1,) + (1,) * (len(extent) - 1 - dim))
    return gain


def split_up(number_of, total, reach, skew):
    portions = [(1 << 20) // math.isqrt(grade ** skew) + 1 for grade in range(2, number_of + 1)]
    spare, holding = total - reach - (number_of - 1), [1] * (number_of - 1)
    while spare > 0:
        free = [i for i in range(number_of - 1) if holding[i] < reach]
        pool, remaining = sum([portions[i] for i in free]), spare
        for i in free:
            addition = min(reach - holding[i], max(1, remaining * portions[i] // pool), spare)
            holding[i] = holding[i] + addition
            spare = spare - addition
    return np.array([reach] + holding)


def ragged(key, count, total, reach, skew):
    if count == 2:
        one = jax.random.randint(key, (), max(1, total - reach), min(reach, total - 1) + 1)
        return jnp.stack([one, total - one])
    tallies = jnp.asarray(split_up(count, total, reach, skew), jnp.int32)
    couples = (count - 1) // 2
    source_of, taker = tallies[1:1 + 2 * couples:2], tallies[2:2 + 2 * couples:2]
    room = jnp.minimum(source_of - 1, reach - taker)
    shifted = jax.random.randint(jax.random.fold_in(key, 1), (couples,), 0, 1 << 20) % (room + 1)
    tallies = tallies.at[1:1 + 2 * couples:2].set(source_of - shifted).at[2:2 + 2 * couples:2].set(taker + shifted)
    return tallies[jax.random.permutation(jax.random.fold_in(key, 2), count)]


def bell_draw(key, dims, scale, bound, split=(), kind=jnp.bfloat16):
    values = jax.random.normal(key, dims, jnp.float32) * scale
    if len(split) > 0:
        values = block_levels(key, dims, split, -0.22, 0.18) * values
    return jnp.clip(values, min=-bound, max=bound).astype(kind)


def setup_inputs(seed: int = 0) -> dict:
    splits = jax.random.split(jax.random.key(seed), 5)
    return {
        "modes": bell_draw(splits[0], (3, NX, YCAP, NZ, M), 1.0, 6.0, ((1, 8), (3, 32))),
        "weights": jnp.clip(jnp.exp(math.log(0.007973615) - 2.3025851 * jax.random.uniform(splits[1], (NX, YCAP, NZ), jnp.float32) ** block_levels(splits[1], (NX, YCAP, NZ), ((0, 8), (2, 32)), -0.2, 0.2)), 0.0007973615, 0.007973615),
        "counts": ragged(splits[2], N_GX * N_GZ, YCAP * DEVICES // 3, YCAP, 2).astype(jnp.int32),
        "mode_index": draw_mode_index(jax.random.fold_in(splits[4], 71), 0),
    }


def reference(modes, weights, counts, mode_index):
    onehot = (jnp.arange(M)[:, None] == mode_index[None, :]).astype(jnp.float32)
    level_ids = jnp.arange(YCAP, dtype=jnp.int32)
    column_ids = jnp.arange(NZ, dtype=jnp.int32)
    highest = lax.Precision.HIGHEST

    def add_plane(running, x_index):
        behind_index = ((x_index - 1 + NX) % NX).astype(jnp.int32)
        ahead_index = ((x_index + 1) % NX).astype(jnp.int32)
        centre = lax.dynamic_index_in_dim(modes, x_index, 1, keepdims=False).astype(jnp.float32)
        behind = lax.dynamic_index_in_dim(modes, behind_index, 1, keepdims=False).astype(jnp.float32)
        forward = lax.dynamic_index_in_dim(modes, ahead_index, 1, keepdims=False).astype(jnp.float32)
        grad_x = 0.5 * (forward - behind)
        padded = jnp.pad(centre, ((0, 0), (1, 1), (0, 0), (0, 0)))
        grad_y = 0.5 * (padded[:, 2:] - padded[:, :-2])
        grad_z = 0.5 * (jnp.roll(centre, -1, axis=2) - jnp.roll(centre, 1, axis=2))
        gradient = jnp.stack([grad_x, grad_y, grad_z])
        picked = jnp.einsum("cyzm,mj->cyzj", centre, onehot, precision=highest)
        advected = jnp.einsum("dyzj,dcyzk->jcyzk", picked, gradient, precision=highest).astype(jnp.bfloat16)
        pencil = (x_index // CX) * N_GZ + column_ids // CZ
        live_mask = level_ids[:, None] < counts[pencil][None, :]
        weight_row = lax.dynamic_index_in_dim(weights, x_index, 0, keepdims=False)
        weighting = jnp.where(live_mask, weight_row, jnp.zeros_like(weight_row))
        tested = (centre * weighting[None, :, :, None]).astype(jnp.bfloat16)
        contrib = jnp.einsum("cyzi,jcyzk->jik", tested.astype(jnp.float32), advected.astype(jnp.float32), precision=highest)
        return running + contrib, None

    zeroed = jnp.zeros((JW, M, M), jnp.float32)
    slices, unused = lax.scan(add_plane, zeroed, jnp.arange(NX, dtype=jnp.int32))
    return slices
```

```python
import functools

import jax
import jax.numpy as jnp
from jax import lax
from jax.experimental import pallas as pl
from jax.experimental.pallas import tpu as pltpu
from jax.sharding import PartitionSpec as P

MESH = pl.DeviceIdType.MESH
BF = jnp.bfloat16
F32 = jnp.float32
M = 128
JW = 16
LV = 128
CZ = 8
ROWS = LV * CZ
PAD = 16
CH = 128
PT = 2 * CH
GRP = 32
STEPS = PT // GRP
HALF = ROWS // 2


def iota(shape, dim):
    return lax.broadcasted_iota(jnp.int32, shape, dim)


def pick_matrix(idx_ref, scales):
    lane = iota((1, M), 1)
    wanted = jnp.zeros((1, M), jnp.int32)
    for j in range(JW):
        wanted = jnp.where(lane % JW == j, idx_ref[j], wanted)
    wanted = jnp.broadcast_to(wanted, (M, M))
    row, col = iota((M, M), 0), iota((M, M), 1)
    blocks = []
    for d, scale in enumerate(scales):
        hit = (row == wanted) & (col // JW == d)
        blocks.append(jnp.where(hit, scale, 0.0).astype(BF))
    return blocks


def weighted_columns(sw, first):
    return jnp.concatenate(
        [jnp.broadcast_to(sw[:, y : y + 1], (CZ, M)) for y in range(first, first + CH // CZ)], axis=0
    )


def dot_part(total, tested, spread, step):
    cols = pl.ds(pl.multiple_of(step * 256, 256), 256)
    total[:, cols] += jnp.dot(tested[...], spread[:, cols], preferred_element_type=F32)


def run_chunks(total, tested, spread, prepare, terms, count):
    for k in range(count + 1):
        if k < count:
            prepare(k, tested[k % 2])

        def step(s, carry, k=k):
            if k > 0:
                dot_part(total, tested[(k - 1) % 2], spread[(k - 1) % 2], s)
            if k < count:
                terms(s, spread[k % 2])
            return carry

        lax.fori_loop(0, STEPS, step, 0)


def local_kernel(
    modes, near, zlo, zhi, sw, idx, total, planes, grad, picks, stencil, sel, tt0, tt1, sp0, sp1, sems
):
    odd = lax.rem(lax.axis_index("gx"), 2)
    sign = jnp.where(odd == 0, 0.5, -0.5).astype(F32)
    copies = []
    for c in range(3):
        for side in range(2):
            which = odd if side == 0 else 1 - odd
            copies.append(
                pltpu.make_async_copy(
                    modes.at[c, which], planes.at[c, side, pl.ds(PAD, ROWS)], sems.at[2 * c + side]
                )
            )
            copies[-1].start()
    for c in range(3):
        for side in range(2):
            planes[c, side, pl.ds(0, PAD), :] = jnp.zeros((PAD, M), BF)
            planes[c, side, pl.ds(PAD + ROWS, PAD), :] = jnp.zeros((PAD, M), BF)
    row, col = iota((2 * CH, 2 * CH), 0), iota((2 * CH, 2 * CH), 1)
    point = lax.rem(row, CH)
    lev, z = point // CZ, lax.rem(point, CZ)
    here = point + PAD
    in_y = jnp.where(col == here + CZ, 1.0, 0.0) - jnp.where(col == here - CZ, 1.0, 0.0)
    ahead = jnp.where(z < CZ - 1, here + 1, 2 * PAD + CH + 16 + lev)
    behind = jnp.where(z > 0, here - 1, 2 * PAD + CH + lev)
    in_z = jnp.where(col == ahead, 1.0, 0.0) - jnp.where(col == behind, 1.0, 0.0)
    stencil[...] = jnp.where(row < CH, in_y, in_z).astype(BF)
    for d, block in enumerate(pick_matrix(idx, (sign, 0.5, 0.5))):
        sel[d * M : (d + 1) * M, :] = block
    total[...] = jnp.zeros_like(total)
    for copy in copies:
        copy.wait()

    def prepare(k, tested):
        first = k * CH
        for side in range(2):
            which = odd if side == 0 else 1 - odd
            wide = weighted_columns(sw[which], k * (CH // CZ))
            rows = slice(side * CH, (side + 1) * CH)
            mine = []
            for c in range(3):
                window = planes[c, side, first : first + CH + 2 * PAD, :]
                lo = zlo[c, which, k * 16 : (k + 1) * 16, :]
                hi = zhi[c, which, k * 16 : (k + 1) * 16, :]
                stacked = jnp.concatenate([window, lo, hi, jnp.zeros((64, M), BF)], axis=0)
                both = jnp.dot(stencil[...], stacked, preferred_element_type=F32)
                grad[3 + c, rows, :] = both[:CH]
                grad[6 + c, rows, :] = both[CH:]
                here = window[PAD : PAD + CH]
                mine.append(here)
                here = here.astype(F32)
                other = planes[c, 1 - side, PAD + first : PAD + first + CH, :].astype(F32)
                if side == 0:
                    grad[c, rows, :] = other
                else:
                    grad[c, rows, :] = near[c, first : first + CH, :].astype(F32) - other
                at = c * PT + side * CH
                tested[:, at : at + CH] = (here * wide).T.astype(BF)
            picks[rows, :] = jnp.dot(jnp.concatenate(mine, axis=1), sel[...], preferred_element_type=F32)

    def terms(s, spread):
        rows = pl.ds(pl.multiple_of(s * GRP, GRP), GRP)
        pk = picks[rows, :]
        g = [grad[q, rows, :] for q in range(9)]
        for j in range(JW):
            px, py, pz = [jnp.broadcast_to(pk[:, d * JW + j : d * JW + j + 1], (GRP, M)) for d in range(3)]
            for c in range(3):
                value = px * g[c] + py * g[3 + c] + pz * g[6 + c]
                at = pl.ds(pl.multiple_of(c * PT + s * GRP, GRP), GRP)
                spread[at, j * M : (j + 1) * M] = value.astype(BF)

    run_chunks(total, (tt0, tt1), (sp0, sp1), prepare, terms, ROWS // CH)


def cross_kernel(
    total_in, mine, far, sw, swfar, idx, out, total, vals, picks, selp, seln, tt0, tt1, sp0, sp1
):
    odd = lax.rem(lax.axis_index("gx"), 2)
    sign = jnp.where(odd == 0, 0.5, -0.5).astype(F32)
    selp[...] = pick_matrix(idx, (sign,))[0]
    seln[...] = pick_matrix(idx, (-sign,))[0]
    total[...] = total_in[...]

    def prepare(k, tested):
        first = (k % 2) * PT
        own = k < 2
        tsrc, vsrc, w, sel = (mine, far, sw, seln) if own else (far, mine, swfar, selp)
        wide = jnp.concatenate(
            [weighted_columns(w[...], (k % 2) * 32), weighted_columns(w[...], (k % 2) * 32 + 16)], axis=0
        )
        for c in range(3):
            here = tsrc[c, first : first + PT, :]
            if c == 0:
                picks[...] = jnp.dot(here, sel[...], preferred_element_type=F32)
            tested[:, c * PT : (c + 1) * PT] = (here.astype(F32) * wide).T.astype(BF)
            vals[c] = vsrc[c, first : first + PT, :].astype(F32)

    def terms(s, spread):
        rows = pl.ds(pl.multiple_of(s * GRP, GRP), GRP)
        pk = picks[rows, :]
        v = [vals[c, rows, :] for c in range(3)]
        for j in range(JW):
            px = jnp.broadcast_to(pk[:, j : j + 1], (GRP, M))
            for c in range(3):
                at = pl.ds(pl.multiple_of(c * PT + s * GRP, GRP), GRP)
                spread[at, j * M : (j + 1) * M] = (px * v[c]).astype(BF)

    run_chunks(total, (tt0, tt1), (sp0, sp1), prepare, terms, 4)
    for q in range(16):
        for low in range(2):
            owner = (q // 4) * 8 + low * 4 + q % 4
            out[q, low * 4 : low * 4 + 4, :] = total[owner * 4 : owner * 4 + 4, :]


def reduce_kernel(part, out, pair, send, got, column, stack, whole, asend, arecv, bsend, brecv, csend, crecv, dsem):
    gx, gz = lax.axis_index("gx"), lax.axis_index("gz")
    core, zh = lax.rem(gx, 2), gx // 2
    x, low, y = gz // 8, lax.rem(gz // 4, 2), lax.rem(gz, 4)
    q, z = x * 4 + y, zh * 2 + low
    partner = (gx + 1 - 2 * core, gz)

    def plane_peer(p):
        return (gx, (p // 4) * 8 + low * 4 + lax.rem(p, 4))

    def column_peer(p):
        return ((p // 2) * 2 + core, x * 8 + lax.rem(p, 2) * 4 + y)

    barrier = pltpu.get_barrier_semaphore()
    peers = [partner]
    peers += [plane_peer(lax.rem(q + d, 16)) for d in range(1, 16)]
    peers += [column_peer(lax.rem(z + d, 8)) for d in range(1, 8)]
    for peer in peers:
        pl.semaphore_signal(barrier, inc=1, device_id=peer, device_id_type=MESH)
    pl.semaphore_wait(barrier, len(peers))

    width = 8 * M
    own = pl.ds(pl.multiple_of(core * width, width), width)
    theirs = pl.ds(pl.multiple_of((1 - core) * width, width), width)

    def pair_copy(g):
        quarter = pl.ds(g * 4, 4)
        return pltpu.make_async_remote_copy(
            src_ref=part.at[quarter, :, theirs],
            dst_ref=pair.at[quarter],
            send_sem=asend.at[g],
            recv_sem=arecv.at[g],
            device_id=partner,
            device_id_type=MESH,
        )

    def plane_copy(dest, slot):
        return pltpu.make_async_remote_copy(
            src_ref=send.at[dest],
            dst_ref=got.at[slot],
            send_sem=bsend.at[dest],
            recv_sem=brecv.at[slot],
            device_id=plane_peer(dest),
            device_id_type=MESH,
        )

    def column_copy(dest, slot):
        return pltpu.make_async_remote_copy(
            src_ref=column.at[lax.rem(dest, 2)],
            dst_ref=stack.at[slot],
            send_sem=csend.at[dest],
            recv_sem=crecv.at[slot],
            device_id=column_peer(dest),
            device_id_type=MESH,
        )

    for g in range(4):
        pair_copy(g).start()
    for g in range(4):
        pair_copy(g).wait_recv()
        for b in range(g * 4, g * 4 + 4):
            send[b] = (part[b, :, own] + pair[b]).astype(BF)

            @pl.when(b != q)
            def _(b=b):
                plane_copy(b, q).start()

    total = send[q].astype(F32)
    for d in range(1, 16):
        p = lax.rem(q + d, 16)
        plane_copy(p, p).wait_recv()
        total = total + got[p].astype(F32)
    column[0] = total[:4]
    column[1] = total[4:]
    for d in (4, 3, 5, 2, 6, 1, 7):
        column_copy(lax.rem(z + d, 8), z).start()
    stack[z] = column[low]
    for d in range(1, 8):
        p = lax.rem(z + d, 8)
        column_copy(p, p).wait_recv()
    mine = stack[0]
    for p in range(1, 8):
        mine = mine + stack[p]
    for j in range(8):
        whole[core * 8 + j] = mine[:, j * M : (j + 1) * M]
    block = whole.at[pl.ds(core * 8, 8)]
    last = pltpu.make_async_remote_copy(
        src_ref=block, dst_ref=block, send_sem=dsem.at[0], recv_sem=dsem.at[1],
        device_id=partner, device_id_type=MESH,
    )
    last.start()
    for g in range(4):
        pair_copy(g).wait_send()
    for d in range(1, 16):
        plane_copy(lax.rem(q + d, 16), q).wait_send()
    for d in range(1, 8):
        column_copy(lax.rem(z + d, 8), z).wait_send()
    last.wait()
    out[...] = whole[...]


VM = pl.BlockSpec(memory_space=pltpu.VMEM)
SM = pl.BlockSpec(memory_space=pltpu.SMEM)
HB = pl.BlockSpec(memory_space=pl.ANY)


def buffers():
    return [pltpu.VMEM((M, 3 * PT), BF)] * 2 + [pltpu.VMEM((3 * PT, JW * M), BF)] * 2


def local(modes, weights, counts, mode_index):
    odd = lax.rem(lax.axis_index("gx"), 2)
    levels = jnp.arange(LV, dtype=jnp.int32)
    wt = jnp.swapaxes(weights, 1, 2)
    sw = jnp.where(levels[None, None, :] < counts[0], wt, jnp.zeros_like(wt))
    flat = modes.reshape(3, 2, ROWS, M)

    count_z = lax.axis_size("gz")
    up = [(i, (i + 1) % count_z) for i in range(count_z)]
    down = [(t, s) for s, t in up]
    zlo = lax.ppermute(modes[:, :, :, CZ - 1, :], "gz", up)
    zhi = lax.ppermute(modes[:, :, :, 0, :], "gz", down)
    count_x = lax.axis_size("gx")
    inside = [(i, i ^ 1) for i in range(count_x)]
    across = [(i, (i + 1) % count_x if i % 2 else (i - 1) % count_x) for i in range(count_x)]
    near = lax.ppermute(lax.dynamic_index_in_dim(flat, 1 - odd, 1, keepdims=False), "gx", inside)
    zero = jnp.zeros((), odd.dtype)
    sent = lax.dynamic_slice(flat, (zero, odd, HALF * (1 - odd), zero), (3, 1, HALF, M))
    swsent = lax.dynamic_slice(sw, (odd, zero, (LV // 2) * (1 - odd)), (1, CZ, LV // 2))[0]
    far = lax.ppermute(sent.reshape(3, HALF, M), "gx", across)
    swfar = lax.ppermute(swsent, "gx", across)

    total = pl.pallas_call(
        local_kernel,
        out_shape=jax.ShapeDtypeStruct((M, JW * M), F32),
        in_specs=[HB, VM, VM, VM, VM, SM],
        out_specs=VM,
        scratch_shapes=[
            pltpu.VMEM((3, 2, ROWS + 2 * PAD, M), BF),
            pltpu.VMEM((9, PT, M), F32),
            pltpu.VMEM((PT, M), F32),
            pltpu.VMEM((2 * CH, 2 * CH), BF),
            pltpu.VMEM((3 * M, M), BF),
            *buffers(),
            pltpu.SemaphoreType.DMA((6,)),
        ],
        compiler_params=pltpu.CompilerParams(vmem_limit_bytes=32 << 20),
        cost_estimate=pl.CostEstimate(flops=6 << 30, bytes_accessed=4 << 20, transcendentals=0),
    )(flat, near, zlo, zhi, sw, mode_index)

    start = HALF * odd
    mine = lax.dynamic_slice(flat, (zero, odd, start, zero), (3, 1, HALF, M)).reshape(3, HALF, M)
    swmine = lax.dynamic_slice(sw, (odd, zero, (LV // 2) * odd), (1, CZ, LV // 2))[0]
    part = pl.pallas_call(
        cross_kernel,
        out_shape=jax.ShapeDtypeStruct((16, 8, JW * M), F32),
        in_specs=[VM, VM, VM, VM, VM, SM],
        out_specs=VM,
        scratch_shapes=[
            pltpu.VMEM((M, JW * M), F32),
            pltpu.VMEM((3, PT, M), F32),
            pltpu.VMEM((PT, M), F32),
            pltpu.VMEM((M, M), BF),
            pltpu.VMEM((M, M), BF),
            *buffers(),
        ],
        compiler_params=pltpu.CompilerParams(vmem_limit_bytes=32 << 20),
        cost_estimate=pl.CostEstimate(flops=2 << 30, bytes_accessed=4 << 20, transcendentals=0),
    )(total, mine, far, swmine, swfar, mode_index)

    return pl.pallas_call(
        reduce_kernel,
        out_shape=jax.ShapeDtypeStruct((JW, 4, M), F32),
        in_specs=[VM],
        out_specs=VM,
        scratch_shapes=[
            pltpu.VMEM((16, 8, 8 * M), F32),
            pltpu.VMEM((16, 8, 8 * M), BF),
            pltpu.VMEM((16, 8, 8 * M), BF),
            pltpu.VMEM((2, 4, 8 * M), F32),
            pltpu.VMEM((8, 4, 8 * M), F32),
            pltpu.VMEM((JW, 4, M), F32),
            pltpu.SemaphoreType.DMA((4,)),
            pltpu.SemaphoreType.DMA((4,)),
            pltpu.SemaphoreType.DMA((16,)),
            pltpu.SemaphoreType.DMA((16,)),
            pltpu.SemaphoreType.DMA((8,)),
            pltpu.SemaphoreType.DMA((8,)),
            pltpu.SemaphoreType.DMA((2,)),
        ],
        compiler_params=pltpu.CompilerParams(collective_id=0, has_side_effects=True),
    )(part)


def solution(mesh):
    placed = (P(None, "gx", None, "gz", None), P("gx", None, "gz"), P(("gx", "gz")), P())
    return jax.shard_map(
        local, mesh=mesh, in_specs=placed, out_specs=P(None, "gz", None), check_vma=False
    )
```

```python
import functools

import jax
import jax.numpy as jnp
from jax import lax
from jax.experimental import pallas as pl
from jax.experimental.pallas import tpu as pltpu
from jax.sharding import PartitionSpec as P

MESH = pl.DeviceIdType.MESH
BF = jnp.bfloat16
F32 = jnp.float32
M = 128
JW = 16
LV = 128
CZ = 8
ROWS = LV * CZ
PAD = 16
CH = 128
PT = 2 * CH
HALF = ROWS // 2


def iota(shape, dim):
    return lax.broadcasted_iota(jnp.int32, shape, dim)


def pick_rows(idx_ref, scales):
    count = len(scales) * JW
    row, col = iota((count, M), 0), iota((count, M), 1)
    wanted = jnp.zeros((count, M), jnp.int32)
    for j in range(JW):
        wanted = jnp.where(row % JW == j, idx_ref[j], wanted)
    blocks = [
        jnp.where((col == wanted) & (row // JW == d), scale, 0.0).astype(BF)
        for d, scale in enumerate(scales)
    ]
    return jnp.concatenate(blocks, axis=1)


def weighted_columns(sw, first, levels):
    return jnp.concatenate(
        [jnp.broadcast_to(sw[:, y : y + 1], (CZ, M)) for y in range(first, first + levels)], axis=0
    )


def stencil_matrix():
    row, col = iota((PT, PT), 0), iota((PT, PT), 1)
    point = lax.rem(col, CH)
    lev, z = point // CZ, lax.rem(point, CZ)
    up = jnp.where(point + CZ < CH, point + CZ, point + CZ + 16)
    down = jnp.where(point >= CZ, point - CZ, CH + 8 + point)
    ahead = jnp.where(z < CZ - 1, point + 1, CH + 48 + lev)
    behind = jnp.where(z > 0, point - 1, CH + 32 + lev)
    plus = jnp.where(col < CH, up, ahead)
    minus = jnp.where(col < CH, down, behind)
    return (jnp.where(row == plus, 1.0, 0.0) - jnp.where(row == minus, 1.0, 0.0)).astype(BF)


def run_chunks(total, tested, spread, prepare, terms, count):
    def dot(step, buffer, k):
        rows = pl.ds(pl.multiple_of(step * 256, 256), 256)
        total[rows, :] += jnp.dot(spread[buffer][...], tested[k % 2][...], preferred_element_type=F32)

    for k in range(count):
        prepare(k)
        if k > 0:
            dot(7, 1, k - 1)
        terms(k, 0, spread[0])

        def body(m, carry, k=k):
            dot(2 * m, 0, k)
            terms(k, 2 * m + 1, spread[1])
            dot(2 * m + 1, 1, k)
            terms(k, 2 * m + 2, spread[0])
            return carry

        lax.fori_loop(0, 3, body, 0)
        dot(6, 0, k)
        terms(k, 7, spread[1])
    dot(7, 1, count - 1)


def local_kernel(
    modes, near, zlo, zhi, sw, idx, total, planes, grad, picks, stencil, sel, tt0, tt1, sp0, sp1, sems
):
    odd = lax.rem(lax.axis_index("gx"), 2)
    sign = jnp.where(odd == 0, 0.5, -0.5).astype(F32)
    copies = []
    for c in range(3):
        for side in range(2):
            which = odd if side == 0 else 1 - odd
            copies.append(
                pltpu.make_async_copy(
                    modes.at[c, which], planes.at[c, side, pl.ds(PAD, ROWS)], sems.at[2 * c + side]
                )
            )
            copies[-1].start()
    for c in range(3):
        for side in range(2):
            planes[c, side, pl.ds(0, PAD), :] = jnp.zeros((PAD, M), BF)
            planes[c, side, pl.ds(PAD + ROWS, PAD), :] = jnp.zeros((PAD, M), BF)
    stencil[...] = stencil_matrix()
    sel[...] = pick_rows(idx, (sign, 0.5, 0.5))
    total[...] = jnp.zeros_like(total)
    for copy in copies:
        copy.wait()

    def prepare(k):
        first = PAD + k * CH
        g, b = grad[k % 2], k % 2
        turned = [[], []]
        for side in range(2):
            which = odd if side == 0 else 1 - odd
            wide = weighted_columns(sw[which], k * (CH // CZ), CH // CZ)
            lanes = slice(side * CH, (side + 1) * CH)
            for c in range(3):
                here = planes[c, side, first : first + CH, :]
                stacked = jnp.concatenate(
                    [
                        here,
                        planes[c, side, first - 16 : first, :],
                        planes[c, side, first + CH : first + CH + 16, :],
                        zlo[c, which, k * 16 : (k + 1) * 16, :],
                        zhi[c, which, k * 16 : (k + 1) * 16, :],
                        jnp.zeros((64, M), BF),
                    ],
                    axis=0,
                ).T
                both = jnp.dot(stacked, stencil[...], preferred_element_type=F32)
                g[3 + c, :, lanes] = both[:, :CH]
                g[6 + c, :, lanes] = both[:, CH:]
                turned[side].append(stacked[:, :CH])
                at = c * PT + side * CH
                (tt0, tt1)[b][at : at + CH, :] = (here.astype(F32) * wide).astype(BF)
            pk = jnp.dot(sel[...], jnp.concatenate(turned[side], axis=0), preferred_element_type=F32)
            for r in range(3 * JW):
                picks[b][r, :, lanes] = jnp.broadcast_to(pk[r : r + 1], (8, CH))
        for c in range(3):
            g[c, :, :CH] = turned[1][c].astype(F32)
            beyond = near[c, k * CH : (k + 1) * CH, :].T
            g[c, :, CH:] = beyond.astype(F32) - turned[0][c].astype(F32)

    def terms(k, step, spread):
        g, pk = grad[k % 2], picks[k % 2]
        scale = []
        for h in range(2):
            p = [pk[d * JW + 2 * step + h] for d in range(3)]
            scale.append([jnp.concatenate([v, v], axis=0) for v in p])
        for c in range(3):
            for t in range(8):
                tile = slice(t * 16, t * 16 + 16)
                gx, gy, gz = g[c, tile, :], g[3 + c, tile, :], g[6 + c, tile, :]
                for h in range(2):
                    px, py, pz = scale[h]
                    value = px * gx + py * gy + pz * gz
                    spread[h * M + t * 16 : h * M + t * 16 + 16, c * PT : (c + 1) * PT] = value.astype(BF)

    run_chunks(total, (tt0, tt1), (sp0, sp1), prepare, terms, ROWS // CH)


def cross_kernel(
    total_in, mine, far, sw, swfar, idx, out, total, vals, picks, selp, seln, tt0, tt1, sp0, sp1
):
    odd = lax.rem(lax.axis_index("gx"), 2)
    sign = jnp.where(odd == 0, 0.5, -0.5).astype(F32)
    selp[...] = pick_rows(idx, (sign,))
    seln[...] = pick_rows(idx, (-sign,))
    total[...] = total_in[...]

    def prepare(k):
        first, b = (k % 2) * PT, k % 2
        own = k < 2
        tsrc, vsrc, w, sel = (mine, far, sw, seln) if own else (far, mine, swfar, selp)
        wide = weighted_columns(w[...], (k % 2) * 32, 32)
        for c in range(3):
            here = tsrc[c, first : first + PT, :]
            if c == 0:
                pk = jnp.dot(sel[...], here.T, preferred_element_type=F32)
                for j in range(JW):
                    picks[b][j] = jnp.broadcast_to(pk[j : j + 1], (16, PT)).astype(BF)
            (tt0, tt1)[b][c * PT : (c + 1) * PT, :] = (here.astype(F32) * wide).astype(BF)
            vals[b][c] = vsrc[c, first : first + PT, :].T

    def terms(k, step, spread):
        v, pk = vals[k % 2], picks[k % 2]
        scale = [pk[2 * step + h] for h in range(2)]
        for c in range(3):
            for t in range(8):
                tile = v[c, t * 16 : t * 16 + 16, :]
                for h in range(2):
                    spread[h * M + t * 16 : h * M + t * 16 + 16, c * PT : (c + 1) * PT] = scale[h] * tile

    run_chunks(total, (tt0, tt1), (sp0, sp1), prepare, terms, 4)
    for j in range(JW):
        block = total[j * M : (j + 1) * M, :].T
        for q in range(16):
            for low in range(2):
                owner = (q // 4) * 8 + low * 4 + q % 4
                out[q, low * 4 : low * 4 + 4, j * M : (j + 1) * M] = block[owner * 4 : owner * 4 + 4]


def reduce_kernel(part, out, pair, send, got, column, stack, whole, asend, arecv, bsend, brecv, csend, crecv, dsem):
    gx, gz = lax.axis_index("gx"), lax.axis_index("gz")
    core, zh = lax.rem(gx, 2), gx // 2
    x, low, y = gz // 8, lax.rem(gz // 4, 2), lax.rem(gz, 4)
    q, z = x * 4 + y, zh * 2 + low
    partner = (gx + 1 - 2 * core, gz)

    def plane_peer(p):
        return (gx, (p // 4) * 8 + low * 4 + lax.rem(p, 4))

    def column_peer(p):
        return ((p // 2) * 2 + core, x * 8 + lax.rem(p, 2) * 4 + y)

    barrier = pltpu.get_barrier_semaphore()
    peers = [partner]
    peers += [plane_peer(lax.rem(q + d, 16)) for d in range(1, 16)]
    peers += [column_peer(lax.rem(z + d, 8)) for d in range(1, 8)]
    for peer in peers:
        pl.semaphore_signal(barrier, inc=1, device_id=peer, device_id_type=MESH)
    pl.semaphore_wait(barrier, len(peers))

    width = 8 * M
    own = pl.ds(pl.multiple_of(core * width, width), width)
    theirs = pl.ds(pl.multiple_of((1 - core) * width, width), width)

    def pair_copy(g):
        quarter = pl.ds(g * 4, 4)
        return pltpu.make_async_remote_copy(
            src_ref=part.at[quarter, :, theirs],
            dst_ref=pair.at[quarter],
            send_sem=asend.at[g],
            recv_sem=arecv.at[g],
            device_id=partner,
            device_id_type=MESH,
        )

    def plane_copy(dest, slot):
        return pltpu.make_async_remote_copy(
            src_ref=send.at[dest],
            dst_ref=got.at[slot],
            send_sem=bsend.at[dest],
            recv_sem=brecv.at[slot],
            device_id=plane_peer(dest),
            device_id_type=MESH,
        )

    def column_copy(dest, slot):
        return pltpu.make_async_remote_copy(
            src_ref=column.at[lax.rem(dest, 2)],
            dst_ref=stack.at[slot],
            send_sem=csend.at[dest],
            recv_sem=crecv.at[slot],
            device_id=column_peer(dest),
            device_id_type=MESH,
        )

    for g in range(4):
        pair_copy(g).start()
    for g in range(4):
        pair_copy(g).wait_recv()
        for b in range(g * 4, g * 4 + 4):
            send[b] = (part[b, :, own] + pair[b]).astype(BF)

            @pl.when(b != q)
            def _(b=b):
                plane_copy(b, q).start()

    total = send[q].astype(F32)
    for d in range(1, 16):
        p = lax.rem(q + d, 16)
        plane_copy(p, p).wait_recv()
        total = total + got[p].astype(F32)
    column[0] = total[:4]
    column[1] = total[4:]
    for d in (4, 3, 5, 2, 6, 1, 7):
        column_copy(lax.rem(z + d, 8), z).start()
    stack[z] = column[low]
    for d in range(1, 8):
        p = lax.rem(z + d, 8)
        column_copy(p, p).wait_recv()
    mine = stack[0]
    for p in range(1, 8):
        mine = mine + stack[p]
    for j in range(8):
        whole[core * 8 + j] = mine[:, j * M : (j + 1) * M]
    block = whole.at[pl.ds(core * 8, 8)]
    last = pltpu.make_async_remote_copy(
        src_ref=block, dst_ref=block, send_sem=dsem.at[0], recv_sem=dsem.at[1],
        device_id=partner, device_id_type=MESH,
    )
    last.start()
    for g in range(4):
        pair_copy(g).wait_send()
    for d in range(1, 16):
        plane_copy(lax.rem(q + d, 16), q).wait_send()
    for d in range(1, 8):
        column_copy(lax.rem(z + d, 8), z).wait_send()
    last.wait()
    out[...] = whole[...]


VM = pl.BlockSpec(memory_space=pltpu.VMEM)
SM = pl.BlockSpec(memory_space=pltpu.SMEM)
HB = pl.BlockSpec(memory_space=pl.ANY)


def buffers():
    return [pltpu.VMEM((3 * PT, M), BF)] * 2 + [pltpu.VMEM((2 * M, 3 * PT), BF)] * 2


def local(modes, weights, counts, mode_index):
    odd = lax.rem(lax.axis_index("gx"), 2)
    levels = jnp.arange(LV, dtype=jnp.int32)
    wt = jnp.swapaxes(weights, 1, 2)
    sw = jnp.where(levels[None, None, :] < counts[0], wt, jnp.zeros_like(wt))
    flat = modes.reshape(3, 2, ROWS, M)

    count_z = lax.axis_size("gz")
    up = [(i, (i + 1) % count_z) for i in range(count_z)]
    down = [(t, s) for s, t in up]
    zlo = lax.ppermute(modes[:, :, :, CZ - 1, :], "gz", up)
    zhi = lax.ppermute(modes[:, :, :, 0, :], "gz", down)
    count_x = lax.axis_size("gx")
    inside = [(i, i ^ 1) for i in range(count_x)]
    across = [(i, (i + 1) % count_x if i % 2 else (i - 1) % count_x) for i in range(count_x)]
    near = lax.ppermute(lax.dynamic_index_in_dim(flat, 1 - odd, 1, keepdims=False), "gx", inside)
    zero = jnp.zeros((), odd.dtype)
    sent = lax.dynamic_slice(flat, (zero, odd, HALF * (1 - odd), zero), (3, 1, HALF, M))
    swsent = lax.dynamic_slice(sw, (odd, zero, (LV // 2) * (1 - odd)), (1, CZ, LV // 2))[0]
    far = lax.ppermute(sent.reshape(3, HALF, M), "gx", across)
    swfar = lax.ppermute(swsent, "gx", across)

    total = pl.pallas_call(
        local_kernel,
        out_shape=jax.ShapeDtypeStruct((JW * M, M), F32),
        in_specs=[HB, VM, VM, VM, VM, SM],
        out_specs=VM,
        scratch_shapes=[
            pltpu.VMEM((3, 2, ROWS + 2 * PAD, M), BF),
            [pltpu.VMEM((9, M, PT), F32)] * 2,
            [pltpu.VMEM((3 * JW, 8, PT), F32)] * 2,
            pltpu.VMEM((PT, PT), BF),
            pltpu.VMEM((3 * JW, 3 * M), BF),
            *buffers(),
            pltpu.SemaphoreType.DMA((6,)),
        ],
        compiler_params=pltpu.CompilerParams(vmem_limit_bytes=32 << 20),
        cost_estimate=pl.CostEstimate(flops=6 << 30, bytes_accessed=4 << 20, transcendentals=0),
    )(flat, near, zlo, zhi, sw, mode_index)

    start = HALF * odd
    mine = lax.dynamic_slice(flat, (zero, odd, start, zero), (3, 1, HALF, M)).reshape(3, HALF, M)
    swmine = lax.dynamic_slice(sw, (odd, zero, (LV // 2) * odd), (1, CZ, LV // 2))[0]
    part = pl.pallas_call(
        cross_kernel,
        out_shape=jax.ShapeDtypeStruct((16, 8, JW * M), F32),
        in_specs=[VM, VM, VM, VM, VM, SM],
        out_specs=VM,
        scratch_shapes=[
            pltpu.VMEM((JW * M, M), F32),
            [pltpu.VMEM((3, M, PT), BF)] * 2,
            [pltpu.VMEM((JW, 16, PT), BF)] * 2,
            pltpu.VMEM((JW, M), BF),
            pltpu.VMEM((JW, M), BF),
            *buffers(),
        ],
        compiler_params=pltpu.CompilerParams(vmem_limit_bytes=32 << 20),
        cost_estimate=pl.CostEstimate(flops=2 << 30, bytes_accessed=4 << 20, transcendentals=0),
    )(total, mine, far, swmine, swfar, mode_index)

    return pl.pallas_call(
        reduce_kernel,
        out_shape=jax.ShapeDtypeStruct((JW, 4, M), F32),
        in_specs=[VM],
        out_specs=VM,
        scratch_shapes=[
            pltpu.VMEM((16, 8, 8 * M), F32),
            pltpu.VMEM((16, 8, 8 * M), BF),
            pltpu.VMEM((16, 8, 8 * M), BF),
            pltpu.VMEM((2, 4, 8 * M), F32),
            pltpu.VMEM((8, 4, 8 * M), F32),
            pltpu.VMEM((JW, 4, M), F32),
            pltpu.SemaphoreType.DMA((4,)),
            pltpu.SemaphoreType.DMA((4,)),
            pltpu.SemaphoreType.DMA((16,)),
            pltpu.SemaphoreType.DMA((16,)),
            pltpu.SemaphoreType.DMA((8,)),
            pltpu.SemaphoreType.DMA((8,)),
            pltpu.SemaphoreType.DMA((2,)),
        ],
        compiler_params=pltpu.CompilerParams(collective_id=0, has_side_effects=True),
    )(part)


def solution(mesh):
    placed = (P(None, "gx", None, "gz", None), P("gx", None, "gz"), P(("gx", "gz")), P())
    return jax.shard_map(
        local, mesh=mesh, in_specs=placed, out_specs=P(None, "gz", None), check_vma=False
    )
```

```python
import functools

import jax
import jax.numpy as jnp
from jax import lax
from jax.experimental import pallas as pl
from jax.experimental.pallas import tpu as pltpu
from jax.sharding import PartitionSpec as P

MESH = pl.DeviceIdType.MESH
BF = jnp.bfloat16
F32 = jnp.float32
M = 128
JW = 16
LV = 128
CZ = 8
ROWS = LV * CZ
PAD = 16
CH = 128
PT = 2 * CH
HALF = ROWS // 2


def iota(shape, dim):
    return lax.broadcasted_iota(jnp.int32, shape, dim)


def pick_rows(idx_ref, scales):
    count = len(scales) * JW
    row, col = iota((count, M), 0), iota((count, M), 1)
    wanted = jnp.zeros((count, M), jnp.int32)
    for j in range(JW):
        wanted = jnp.where(row % JW == j, idx_ref[j], wanted)
    blocks = [
        jnp.where((col == wanted) & (row // JW == d), scale, 0.0).astype(BF)
        for d, scale in enumerate(scales)
    ]
    return jnp.concatenate(blocks, axis=1)


def weighted_columns(sw, first, levels):
    return jnp.concatenate(
        [jnp.broadcast_to(sw[:, y : y + 1], (CZ, M)) for y in range(first, first + levels)], axis=0
    )


def stencil_matrix():
    row, col = iota((PT, PT), 0), iota((PT, PT), 1)
    point = lax.rem(col, CH)
    lev, z = point // CZ, lax.rem(point, CZ)
    up = jnp.where(point + CZ < CH, point + CZ, point + CZ + 16)
    down = jnp.where(point >= CZ, point - CZ, CH + 8 + point)
    ahead = jnp.where(z < CZ - 1, point + 1, CH + 48 + lev)
    behind = jnp.where(z > 0, point - 1, CH + 32 + lev)
    plus = jnp.where(col < CH, up, ahead)
    minus = jnp.where(col < CH, down, behind)
    return (jnp.where(row == plus, 1.0, 0.0) - jnp.where(row == minus, 1.0, 0.0)).astype(BF)


def select_rows():
    row, col = iota((32, CH), 0), iota((32, CH), 1)
    return jnp.where(col == lax.rem(row, 16) * CZ + (row // 16) * (CZ - 1), 1.0, 0.0).astype(BF)


def local_kernel(
    modes, weights, counts, idx, out,
    total, planes, near, far, zsend, zgot, sw, swfar, turned, cross_tested, grads, picks, spread, stencil, sel, self_,
    local_sem, near_s, near_r, far_s, far_r, z_s, z_r, w_sem,
):
    gx, gz = lax.axis_index("gx"), lax.axis_index("gz")
    odd = lax.rem(gx, 2)
    sign = jnp.where(odd == 0, 0.5, -0.5).astype(F32)
    near_peer = (gx + 1 - 2 * odd, gz)
    far_peer = (lax.rem(gx + 7 + 2 * odd, 8), gz)
    z_peers = ((gx, lax.rem(gz + 31, 32)), (gx, lax.rem(gz + 1, 32)))

    copies = []
    for c in range(3):
        for side in range(2):
            which = odd if side == 0 else 1 - odd
            copies.append(
                pltpu.make_async_copy(
                    modes.at[c, which], planes.at[c, side, pl.ds(PAD, ROWS)], local_sem.at[2 * c + side]
                )
            )
            copies[-1].start()
    barrier = pltpu.get_barrier_semaphore()
    for peer in (near_peer, far_peer, *z_peers):
        pl.semaphore_signal(barrier, inc=1, device_id=peer, device_id_type=MESH)
    for c in range(3):
        for side in range(2):
            planes[c, side, pl.ds(0, PAD), :] = jnp.zeros((PAD, M), BF)
            planes[c, side, pl.ds(PAD + ROWS, PAD), :] = jnp.zeros((PAD, M), BF)
    for side in range(2):
        which = odd if side == 0 else 1 - odd
        w = weights[which]
        sw[side] = jnp.where(iota((CZ, LV), 1) < counts[0], w, jnp.zeros_like(w))
    stencil[...] = stencil_matrix()
    sel[...] = pick_rows(idx, (sign, 0.5, 0.5))
    self_[...] = pick_rows(idx, (sign,))
    total[...] = jnp.zeros_like(total)
    spread[1][...] = jnp.zeros_like(spread[1])
    ends = select_rows()
    for copy in copies:
        copy.wait()
    pl.semaphore_wait(barrier, 4)

    def block_of(t):
        return lax.rem(t + 4 * (1 - odd), 8)

    def rows_of(k):
        return pl.ds(pl.multiple_of(PAD + k * CH, 16), CH)

    def near_copy(k):
        return pltpu.make_async_remote_copy(
            src_ref=planes.at[:, 1, rows_of(k)], dst_ref=near.at[k],
            send_sem=near_s.at[k], recv_sem=near_r.at[k], device_id=near_peer, device_id_type=MESH,
        )

    def far_copy(p):
        return pltpu.make_async_remote_copy(
            src_ref=planes.at[:, 0, rows_of(p + 4 * (1 - odd))], dst_ref=far.at[p],
            send_sem=far_s.at[p], recv_sem=far_r.at[p], device_id=far_peer, device_id_type=MESH,
        )

    def z_copy(direction, k):
        return pltpu.make_async_remote_copy(
            src_ref=zsend.at[direction, k], dst_ref=zgot.at[direction, k],
            send_sem=z_s.at[direction, k], recv_sem=z_r.at[direction, k],
            device_id=z_peers[direction], device_id_type=MESH,
        )

    weight_copy = pltpu.make_async_remote_copy(
        src_ref=sw.at[0], dst_ref=swfar, send_sem=w_sem.at[0], recv_sem=w_sem.at[1],
        device_id=far_peer, device_id_type=MESH,
    )
    for t in range(8):
        near_copy(lax.rem(t + 4 * odd, 8)).start()
        if t < 4:
            far_copy(t).start()

    def send_edges(t, carry):
        k = block_of(t)
        for c in range(3):
            for side in range(2):
                edge = jnp.dot(ends, planes[c, side, rows_of(k), :], preferred_element_type=F32).astype(BF)
                at = (2 * c + side) * 16
                zsend[0, k, at : at + 16, :] = edge[:16]
                zsend[1, k, at : at + 16, :] = edge[16:]
        z_copy(0, k).start()
        z_copy(1, k).start()
        return carry

    lax.fori_loop(0, 8, send_edges, 0)
    weight_copy.start()
    for k in range(8):
        for side in range(2):
            wide = weighted_columns(sw[side], k * 16, 16)
            for c in range(3):
                here = planes[c, side, PAD + k * CH : PAD + (k + 1) * CH, :].astype(F32)
                at = c * PT + side * CH
                turned[k, :, at : at + CH] = (here * wide).astype(BF).T

    def dot(step, buffer, tested):
        cols = pl.ds(pl.multiple_of(step * 256, 256), 256)
        total[:, cols] += lax.dot_general(
            tested, spread[buffer][...], (((1,), (1,)), ((), ())), preferred_element_type=F32
        )

    def run(first, tested, terms):
        first()
        terms(0, spread[0])

        def body(m, carry):
            dot(2 * m, 0, tested())
            terms(2 * m + 1, spread[1])
            dot(2 * m + 1, 1, tested())
            terms(2 * m + 2, spread[0])
            return carry

        lax.fori_loop(0, 3, body, 0)
        dot(6, 0, tested())
        terms(7, spread[1])

    def prepare(t, b, with_far):
        k = block_of(t)
        g = grads[b]
        flipped = [[], []]
        for side in range(2):
            lanes = slice(side * CH, (side + 1) * CH)
            for c in range(3):
                at = (2 * c + side) * 16
                stacked = jnp.concatenate(
                    [
                        planes[c, side, rows_of(k), :],
                        planes[c, side, pl.ds(pl.multiple_of(k * CH, 16), 16), :],
                        planes[c, side, pl.ds(pl.multiple_of(PAD + (k + 1) * CH, 16), 16), :],
                        zgot[1, k, at : at + 16, :],
                        zgot[0, k, at : at + 16, :],
                        jnp.zeros((64, M), BF),
                    ],
                    axis=0,
                ).T
                both = jnp.dot(stacked, stencil[...], preferred_element_type=F32)
                g[3 + c, :, lanes] = both[:, :CH]
                g[6 + c, :, lanes] = both[:, CH:]
                flipped[side].append(stacked[:, :CH])
            pk = jnp.dot(sel[...], jnp.concatenate(flipped[side], axis=0), preferred_element_type=F32)
            for r in range(3 * JW):
                picks[b][r, :, lanes] = jnp.broadcast_to(pk[r : r + 1], (8, CH))
        for c in range(3):
            inner = flipped[1][c].astype(F32)
            if with_far:
                inner = inner - far[t - 4, c].T.astype(F32)
            g[c, :, :CH] = inner
            g[c, :, CH:] = near[k, c].T.astype(F32) - flipped[0][c].astype(F32)

    def terms(b, step, target):
        g, pk = grads[b], picks[b]
        scale = []
        for h in range(2):
            p = [pk[d * JW + 2 * step + h] for d in range(3)]
            scale.append([jnp.concatenate([v, v], axis=0) for v in p])
        for c in range(3):
            for u in range(8):
                tile = slice(u * 16, u * 16 + 16)
                gx_, gy_, gz_ = g[c, tile, :], g[3 + c, tile, :], g[6 + c, tile, :]
                for h in range(2):
                    px, py, pz = scale[h]
                    value = px * gx_ + py * gy_ + pz * gz_
                    target[h * M + u * 16 : h * M + u * 16 + 16, c * PT : (c + 1) * PT] = value.astype(BF)

    def pair(u, carry, with_far):
        for t in (2 * u, 2 * u + 1):
            near_copy(block_of(t)).wait_recv()
            z_copy(0, block_of(t)).wait_recv()
            z_copy(1, block_of(t)).wait_recv()
            if with_far:
                far_copy(t - 4).wait_recv()
        for b in range(2):
            t = 2 * u + b
            before = block_of(lax.rem(t + 7, 8))

            def first(t=t, b=b, before=before):
                prepare(t, b, with_far)
                dot(7, 1, turned[before])

            run(first, lambda t=t: turned[block_of(t)], functools.partial(terms, b))
        return carry

    lax.fori_loop(0, 2, functools.partial(pair, with_far=False), 0)
    lax.fori_loop(2, 4, functools.partial(pair, with_far=True), 0)

    weight_copy.wait_recv()
    foreign = swfar[...]
    foreign = jnp.where(odd == 1, pltpu.roll(foreign, LV // 2, 1), foreign)

    def prepare_cross(v):
        wide = [weighted_columns(foreign, v * 32 + 16 * h, 16) for h in range(2)]
        pk = []
        for h in range(2):
            mine = 2 * v + h + 4 * odd
            for c in range(3):
                here = far[2 * v + h, c]
                if c == 0:
                    pk.append(jnp.dot(self_[...], here.T, preferred_element_type=F32).astype(BF))
                at = c * PT + h * CH
                cross_tested[v, :, at : at + CH] = (here.astype(F32) * wide[h]).astype(BF).T
                grads[v][c, :, h * CH : (h + 1) * CH] = planes[c, 0, rows_of(mine), :].T.astype(F32)
            for j in range(JW):
                picks[v][j, :, h * CH : (h + 1) * CH] = jnp.broadcast_to(
                    pk[h][j : j + 1].astype(F32), (8, CH)
                )

    def cross_terms(v, step, target):
        scale = []
        for h in range(2):
            p = picks[v][2 * step + h].astype(BF)
            scale.append(jnp.concatenate([p, p], axis=0))
        for c in range(3):
            for u in range(8):
                tile = grads[v][c, u * 16 : u * 16 + 16, :].astype(BF)
                for h in range(2):
                    target[h * M + u * 16 : h * M + u * 16 + 16, c * PT : (c + 1) * PT] = scale[h] * tile

    for v in range(2):

        def first(v=v):
            prepare_cross(v)
            dot(7, 1, turned[block_of(7)] if v == 0 else cross_tested[0])

        run(first, lambda v=v: cross_tested[v], functools.partial(cross_terms, v))
    dot(7, 1, cross_tested[1])

    for q in range(16):
        for low in range(2):
            owner = (q // 4) * 8 + low * 4 + q % 4
            out[q, low * 4 : low * 4 + 4, :] = total[owner * 4 : owner * 4 + 4, :]
    for k in range(8):
        near_copy(k).wait_send()
        z_copy(0, k).wait_send()
        z_copy(1, k).wait_send()
        if k < 4:
            far_copy(k).wait_send()
    weight_copy.wait_send()


def reduce_kernel(part, out, pair, send, got, column, stack, whole, asend, arecv, bsend, brecv, csend, crecv, dsem):
    gx, gz = lax.axis_index("gx"), lax.axis_index("gz")
    core, zh = lax.rem(gx, 2), gx // 2
    x, low, y = gz // 8, lax.rem(gz // 4, 2), lax.rem(gz, 4)
    q, z = x * 4 + y, zh * 2 + low
    partner = (gx + 1 - 2 * core, gz)

    def plane_peer(p):
        return (gx, (p // 4) * 8 + low * 4 + lax.rem(p, 4))

    def column_peer(p):
        return ((p // 2) * 2 + core, x * 8 + lax.rem(p, 2) * 4 + y)

    barrier = pltpu.get_barrier_semaphore()
    peers = [partner]
    peers += [plane_peer(lax.rem(q + d, 16)) for d in range(1, 16)]
    peers += [column_peer(lax.rem(z + d, 8)) for d in range(1, 8)]
    for peer in peers:
        pl.semaphore_signal(barrier, inc=1, device_id=peer, device_id_type=MESH)
    pl.semaphore_wait(barrier, len(peers))

    width = 8 * M
    own = pl.ds(pl.multiple_of(core * width, width), width)
    theirs = pl.ds(pl.multiple_of((1 - core) * width, width), width)

    def pair_copy(g):
        quarter = pl.ds(g * 4, 4)
        return pltpu.make_async_remote_copy(
            src_ref=part.at[quarter, :, theirs],
            dst_ref=pair.at[quarter],
            send_sem=asend.at[g],
            recv_sem=arecv.at[g],
            device_id=partner,
            device_id_type=MESH,
        )

    def plane_copy(dest, slot):
        return pltpu.make_async_remote_copy(
            src_ref=send.at[dest],
            dst_ref=got.at[slot],
            send_sem=bsend.at[dest],
            recv_sem=brecv.at[slot],
            device_id=plane_peer(dest),
            device_id_type=MESH,
        )

    def column_copy(dest, slot):
        return pltpu.make_async_remote_copy(
            src_ref=column.at[lax.rem(dest, 2)],
            dst_ref=stack.at[slot],
            send_sem=csend.at[dest],
            recv_sem=crecv.at[slot],
            device_id=column_peer(dest),
            device_id_type=MESH,
        )

    for g in range(4):
        pair_copy(g).start()
    for g in range(4):
        pair_copy(g).wait_recv()
        for b in range(g * 4, g * 4 + 4):
            send[b] = (part[b, :, own] + pair[b]).astype(BF)

            @pl.when(b != q)
            def _(b=b):
                plane_copy(b, q).start()

    total = send[q].astype(F32)
    for d in range(1, 16):
        p = lax.rem(q + d, 16)
        plane_copy(p, p).wait_recv()
        total = total + got[p].astype(F32)
    column[0] = total[:4]
    column[1] = total[4:]
    for d in (4, 3, 5, 2, 6, 1, 7):
        column_copy(lax.rem(z + d, 8), z).start()
    stack[z] = column[low]
    for d in range(1, 8):
        p = lax.rem(z + d, 8)
        column_copy(p, p).wait_recv()
    mine = stack[0]
    for p in range(1, 8):
        mine = mine + stack[p]
    for j in range(8):
        whole[core * 8 + j] = mine[:, j * M : (j + 1) * M]
    block = whole.at[pl.ds(core * 8, 8)]
    last = pltpu.make_async_remote_copy(
        src_ref=block, dst_ref=block, send_sem=dsem.at[0], recv_sem=dsem.at[1],
        device_id=partner, device_id_type=MESH,
    )
    last.start()
    for g in range(4):
        pair_copy(g).wait_send()
    for d in range(1, 16):
        plane_copy(lax.rem(q + d, 16), q).wait_send()
    for d in range(1, 8):
        column_copy(lax.rem(z + d, 8), z).wait_send()
    last.wait()
    out[...] = whole[...]


VM = pl.BlockSpec(memory_space=pltpu.VMEM)
SM = pl.BlockSpec(memory_space=pltpu.SMEM)
HB = pl.BlockSpec(memory_space=pl.ANY)


def local(modes, weights, counts, mode_index):
    part = pl.pallas_call(
        local_kernel,
        out_shape=jax.ShapeDtypeStruct((16, 8, JW * M), F32),
        in_specs=[HB, VM, SM, SM],
        out_specs=VM,
        scratch_shapes=[
            pltpu.VMEM((M, JW * M), F32),
            pltpu.VMEM((3, 2, ROWS + 2 * PAD, M), BF),
            pltpu.VMEM((8, 3, CH, M), BF),
            pltpu.VMEM((4, 3, CH, M), BF),
            pltpu.VMEM((2, 8, 96, M), BF),
            pltpu.VMEM((2, 8, 96, M), BF),
            pltpu.VMEM((2, CZ, LV), F32),
            pltpu.VMEM((CZ, LV), F32),
            pltpu.VMEM((8, M, 3 * PT), BF),
            pltpu.VMEM((2, M, 3 * PT), BF),
            [pltpu.VMEM((9, M, PT), F32)] * 2,
            [pltpu.VMEM((3 * JW, 8, PT), F32)] * 2,
            [pltpu.VMEM((2 * M, 3 * PT), BF)] * 2,
            pltpu.VMEM((PT, PT), BF),
            pltpu.VMEM((3 * JW, 3 * M), BF),
            pltpu.VMEM((JW, M), BF),
            pltpu.SemaphoreType.DMA((6,)),
            pltpu.SemaphoreType.DMA((8,)),
            pltpu.SemaphoreType.DMA((8,)),
            pltpu.SemaphoreType.DMA((4,)),
            pltpu.SemaphoreType.DMA((4,)),
            pltpu.SemaphoreType.DMA((2, 8)),
            pltpu.SemaphoreType.DMA((2, 8)),
            pltpu.SemaphoreType.DMA((2,)),
        ],
        compiler_params=pltpu.CompilerParams(
            vmem_limit_bytes=40 << 20, collective_id=1, has_side_effects=True
        ),
    )(modes.reshape(3, 2, ROWS, M), jnp.swapaxes(weights, 1, 2), counts, mode_index)

    return pl.pallas_call(
        reduce_kernel,
        out_shape=jax.ShapeDtypeStruct((JW, 4, M), F32),
        in_specs=[VM],
        out_specs=VM,
        scratch_shapes=[
            pltpu.VMEM((16, 8, 8 * M), F32),
            pltpu.VMEM((16, 8, 8 * M), BF),
            pltpu.VMEM((16, 8, 8 * M), BF),
            pltpu.VMEM((2, 4, 8 * M), F32),
            pltpu.VMEM((8, 4, 8 * M), F32),
            pltpu.VMEM((JW, 4, M), F32),
            pltpu.SemaphoreType.DMA((4,)),
            pltpu.SemaphoreType.DMA((4,)),
            pltpu.SemaphoreType.DMA((16,)),
            pltpu.SemaphoreType.DMA((16,)),
            pltpu.SemaphoreType.DMA((8,)),
            pltpu.SemaphoreType.DMA((8,)),
            pltpu.SemaphoreType.DMA((2,)),
        ],
        compiler_params=pltpu.CompilerParams(collective_id=0, has_side_effects=True),
    )(part)


def solution(mesh):
    placed = (P(None, "gx", None, "gz", None), P("gx", None, "gz"), P(("gx", "gz")), P())
    return jax.shard_map(
        local, mesh=mesh, in_specs=placed, out_specs=P(None, "gz", None), check_vma=False
    )
```

```python
import functools

import jax
import jax.numpy as jnp
from jax import lax
from jax.experimental import pallas as pl
from jax.experimental.pallas import tpu as pltpu
from jax.sharding import PartitionSpec as P

MESH = pl.DeviceIdType.MESH
BF = jnp.bfloat16
F32 = jnp.float32
M = 128
JW = 16
LV = 128
CZ = 8
ROWS = LV * CZ
PAD = 16
CH = 128
PT = 2 * CH
HALF = ROWS // 2


def iota(shape, dim):
    return lax.broadcasted_iota(jnp.int32, shape, dim)


def pick_rows(idx_ref, scales):
    count = len(scales) * JW
    row, col = iota((count, M), 0), iota((count, M), 1)
    wanted = jnp.zeros((count, M), jnp.int32)
    for j in range(JW):
        wanted = jnp.where(row % JW == j, idx_ref[j], wanted)
    blocks = [
        jnp.where((col == wanted) & (row // JW == d), scale, 0.0).astype(BF)
        for d, scale in enumerate(scales)
    ]
    return jnp.concatenate(blocks, axis=1)


def weighted_columns(sw, first, levels):
    return jnp.concatenate(
        [jnp.broadcast_to(sw[:, y : y + 1], (CZ, M)) for y in range(first, first + levels)], axis=0
    )


def stencil_matrix():
    row, col = iota((PT, PT), 0), iota((PT, PT), 1)
    point = lax.rem(col, CH)
    lev, z = point // CZ, lax.rem(point, CZ)
    up = jnp.where(point + CZ < CH, point + CZ, point + CZ + 16)
    down = jnp.where(point >= CZ, point - CZ, CH + 8 + point)
    ahead = jnp.where(z < CZ - 1, point + 1, CH + 48 + lev)
    behind = jnp.where(z > 0, point - 1, CH + 32 + lev)
    plus = jnp.where(col < CH, up, ahead)
    minus = jnp.where(col < CH, down, behind)
    return (jnp.where(row == plus, 1.0, 0.0) - jnp.where(row == minus, 1.0, 0.0)).astype(BF)


def select_rows():
    row, col = iota((32, CH), 0), iota((32, CH), 1)
    return jnp.where(col == lax.rem(row, 16) * CZ + (row // 16) * (CZ - 1), 1.0, 0.0).astype(BF)


def place():
    gx, gz = lax.axis_index("gx"), lax.axis_index("gz")
    core, zh = lax.rem(gx, 2), gx // 2
    x, low, y = gz // 8, lax.rem(gz // 4, 2), lax.rem(gz, 4)
    return gx, gz, core, x, low, y, x * 4 + y, zh * 2 + low


def plane_peer(p):
    gx, _, _, _, low, _, _, _ = place()
    return (gx, (p // 4) * 8 + low * 4 + lax.rem(p, 4))


def column_peer(p):
    _, _, core, x, _, y, _, _ = place()
    return ((p // 2) * 2 + core, x * 8 + lax.rem(p, 2) * 4 + y)


def reduction_peers():
    _, _, _, _, _, _, q, z = place()
    return [plane_peer(lax.rem(q + d, 16)) for d in range(1, 16)] + [
        column_peer(lax.rem(z + d, 8)) for d in range(1, 8)
    ]


def reduce_parts(
    total, out, part, pair, send, got, column, stack, whole, asend, arecv, bsend, brecv, csend, crecv, dsem
):
    gx, gz, core, x, low, y, q, z = place()
    partner = (gx + 1 - 2 * core, gz)

    width = 8 * M
    own = pl.ds(pl.multiple_of(core * width, width), width)
    theirs = pl.ds(pl.multiple_of((1 - core) * width, width), width)

    def pair_copy(g):
        quarter = pl.ds(g * 4, 4)
        return pltpu.make_async_remote_copy(
            src_ref=part.at[quarter, :, theirs],
            dst_ref=pair.at[quarter],
            send_sem=asend.at[g],
            recv_sem=arecv.at[g],
            device_id=partner,
            device_id_type=MESH,
        )

    def plane_copy(dest, slot):
        return pltpu.make_async_remote_copy(
            src_ref=send.at[dest],
            dst_ref=got.at[slot],
            send_sem=bsend.at[dest],
            recv_sem=brecv.at[slot],
            device_id=plane_peer(dest),
            device_id_type=MESH,
        )

    def column_copy(dest, slot):
        return pltpu.make_async_remote_copy(
            src_ref=column.at[lax.rem(dest, 2)],
            dst_ref=stack.at[slot],
            send_sem=csend.at[dest],
            recv_sem=crecv.at[slot],
            device_id=column_peer(dest),
            device_id_type=MESH,
        )

    for g in range(4):
        for b in range(g * 4, g * 4 + 4):
            for half in range(2):
                owner = (b // 4) * 8 + half * 4 + b % 4
                part[b, half * 4 : half * 4 + 4, :] = total[owner * 4 : owner * 4 + 4, :]
        pair_copy(g).start()
    for g in range(4):
        pair_copy(g).wait_recv()
        for b in range(g * 4, g * 4 + 4):
            send[b] = (part[b, :, own] + pair[b]).astype(BF)

            @pl.when(b != q)
            def _(b=b):
                plane_copy(b, q).start()

    mine = send[q].astype(F32)
    for d in range(1, 16):
        p = lax.rem(q + d, 16)
        plane_copy(p, p).wait_recv()
        mine = mine + got[p].astype(F32)
    column[0] = mine[:4]
    column[1] = mine[4:]
    for d in (4, 3, 5, 2, 6, 1, 7):
        column_copy(lax.rem(z + d, 8), z).start()
    stack[z] = column[low]
    for d in range(1, 8):
        p = lax.rem(z + d, 8)
        column_copy(p, p).wait_recv()
    mine = stack[0]
    for p in range(1, 8):
        mine = mine + stack[p]
    for j in range(8):
        whole[core * 8 + j] = mine[:, j * M : (j + 1) * M]
    block = whole.at[pl.ds(core * 8, 8)]
    last = pltpu.make_async_remote_copy(
        src_ref=block, dst_ref=block, send_sem=dsem.at[0], recv_sem=dsem.at[1],
        device_id=partner, device_id_type=MESH,
    )
    last.start()
    last.wait_recv()
    out[...] = whole[...]

    def finish():
        for g in range(4):
            pair_copy(g).wait_send()
        for d in range(1, 16):
            plane_copy(lax.rem(q + d, 16), q).wait_send()
        for d in range(1, 8):
            column_copy(lax.rem(z + d, 8), z).wait_send()
        last.wait_send()

    return finish


def local_kernel(
    modes, weights, counts, idx, out,
    weights_in, total, planes, near, far, zsend, zgot, sw, swfar, turned, cross_tested, grads, picks, spread, stencil, sel, self_,
    local_sem, near_s, near_r, far_s, far_r, z_s, z_r, w_sem, *reduction,
):
    gx, gz = lax.axis_index("gx"), lax.axis_index("gz")
    odd = lax.rem(gx, 2)
    sign = jnp.where(odd == 0, 0.5, -0.5).astype(F32)
    near_peer = (gx + 1 - 2 * odd, gz)
    far_peer = (lax.rem(gx + 7 + 2 * odd, 8), gz)
    z_peers = ((gx, lax.rem(gz + 31, 32)), (gx, lax.rem(gz + 1, 32)))

    barrier = pltpu.get_barrier_semaphore()
    peers = [near_peer, far_peer, *z_peers, *reduction_peers()]
    for peer in peers:
        pl.semaphore_signal(barrier, inc=1, device_id=peer, device_id_type=MESH)
    small = [pltpu.make_async_copy(weights, weights_in, local_sem.at[6])]
    copies = []
    for c in range(3):
        for side in range(2):
            which = odd if side == 0 else 1 - odd
            copies.append(
                pltpu.make_async_copy(
                    modes.at[c, which], planes.at[c, side, pl.ds(PAD, ROWS)], local_sem.at[2 * c + side]
                )
            )
    for copy in (*small, *copies):
        copy.start()
    for c in range(3):
        for side in range(2):
            planes[c, side, pl.ds(0, PAD), :] = jnp.zeros((PAD, M), BF)
            planes[c, side, pl.ds(PAD + ROWS, PAD), :] = jnp.zeros((PAD, M), BF)
    for copy in small:
        copy.wait()
    for side in range(2):
        which = odd if side == 0 else 1 - odd
        w = weights_in[which]
        sw[side] = jnp.where(iota((CZ, LV), 1) < counts[0], w, jnp.zeros_like(w))
    stencil[...] = stencil_matrix()
    sel[...] = pick_rows(idx, (sign, 0.5, 0.5))
    self_[...] = pick_rows(idx, (sign,))
    total[...] = jnp.zeros_like(total)
    spread[1][...] = jnp.zeros_like(spread[1])
    ends = select_rows()
    for copy in copies:
        copy.wait()

    def block_of(t):
        return lax.rem(t + 4 * (1 - odd), 8)

    def rows_of(k):
        return pl.ds(pl.multiple_of(PAD + k * CH, 16), CH)

    def near_copy(k):
        return pltpu.make_async_remote_copy(
            src_ref=planes.at[:, 1, rows_of(k)], dst_ref=near.at[k],
            send_sem=near_s.at[k], recv_sem=near_r.at[k], device_id=near_peer, device_id_type=MESH,
        )

    def far_copy(p):
        return pltpu.make_async_remote_copy(
            src_ref=planes.at[:, 0, rows_of(p + 4 * (1 - odd))], dst_ref=far.at[p],
            send_sem=far_s.at[p], recv_sem=far_r.at[p], device_id=far_peer, device_id_type=MESH,
        )

    def z_copy(direction, k):
        return pltpu.make_async_remote_copy(
            src_ref=zsend.at[direction, k], dst_ref=zgot.at[direction, k],
            send_sem=z_s.at[direction, k], recv_sem=z_r.at[direction, k],
            device_id=z_peers[direction], device_id_type=MESH,
        )

    weight_copy = pltpu.make_async_remote_copy(
        src_ref=sw.at[0], dst_ref=swfar, send_sem=w_sem.at[0], recv_sem=w_sem.at[1],
        device_id=far_peer, device_id_type=MESH,
    )

    def send_edges(t, carry):
        k = block_of(t)
        for c in range(3):
            for side in range(2):
                edge = jnp.dot(ends, planes[c, side, rows_of(k), :], preferred_element_type=F32).astype(BF)
                at = (2 * c + side) * 16
                zsend[0, k, at : at + 16, :] = edge[:16]
                zsend[1, k, at : at + 16, :] = edge[16:]
        return carry

    lax.fori_loop(0, 8, send_edges, 0)
    pl.semaphore_wait(barrier, len(peers))
    for t in range(8):
        near_copy(lax.rem(t + 4 * odd, 8)).start()
        z_copy(0, block_of(t)).start()
        z_copy(1, block_of(t)).start()
    weight_copy.start()
    for k in range(8):
        for side in range(2):
            wide = weighted_columns(sw[side], k * 16, 16)
            for c in range(3):
                here = planes[c, side, PAD + k * CH : PAD + (k + 1) * CH, :].astype(F32)
                at = c * PT + side * CH
                turned[k, :, at : at + CH] = (here * wide).astype(BF).T

    far_copy(0).start()
    far_copy(1).start()

    def dot(step, buffer, tested):
        cols = pl.ds(pl.multiple_of(step * 256, 256), 256)
        total[:, cols] += lax.dot_general(
            tested, spread[buffer][...], (((1,), (1,)), ((), ())), preferred_element_type=F32
        )

    def run(first, tested, terms):
        first()
        terms(0, spread[0])

        def body(m, carry):
            dot(2 * m, 0, tested())
            terms(2 * m + 1, spread[1])
            dot(2 * m + 1, 1, tested())
            terms(2 * m + 2, spread[0])
            return carry

        lax.fori_loop(0, 3, body, 0)
        dot(6, 0, tested())
        terms(7, spread[1])

    def prepare(t, b, with_far):
        k = block_of(t)
        g = grads[b]
        flipped = [[], []]
        for side in range(2):
            lanes = slice(side * CH, (side + 1) * CH)
            for c in range(3):
                at = (2 * c + side) * 16
                stacked = jnp.concatenate(
                    [
                        planes[c, side, rows_of(k), :],
                        planes[c, side, pl.ds(pl.multiple_of(k * CH, 16), 16), :],
                        planes[c, side, pl.ds(pl.multiple_of(PAD + (k + 1) * CH, 16), 16), :],
                        zgot[1, k, at : at + 16, :],
                        zgot[0, k, at : at + 16, :],
                        jnp.zeros((64, M), BF),
                    ],
                    axis=0,
                ).T
                both = jnp.dot(stacked, stencil[...], preferred_element_type=F32)
                g[3 + c, :, lanes] = both[:, :CH]
                g[6 + c, :, lanes] = both[:, CH:]
                flipped[side].append(stacked[:, :CH])
            pk = jnp.dot(sel[...], jnp.concatenate(flipped[side], axis=0), preferred_element_type=F32)
            for r in range(3 * JW):
                picks[b][r, :, lanes] = jnp.broadcast_to(pk[r : r + 1], (8, CH))
        for c in range(3):
            inner = flipped[1][c].astype(F32)
            if with_far:
                inner = inner - far[t - 4, c].T.astype(F32)
            g[c, :, :CH] = inner
            g[c, :, CH:] = near[k, c].T.astype(F32) - flipped[0][c].astype(F32)

    def terms(b, step, target):
        g, pk = grads[b], picks[b]
        scale = []
        for h in range(2):
            p = [pk[d * JW + 2 * step + h] for d in range(3)]
            scale.append([jnp.concatenate([v, v], axis=0) for v in p])
        for c in range(3):
            for u in range(8):
                tile = slice(u * 16, u * 16 + 16)
                gx_, gy_, gz_ = g[c, tile, :], g[3 + c, tile, :], g[6 + c, tile, :]
                for h in range(2):
                    px, py, pz = scale[h]
                    value = px * gx_ + py * gy_ + pz * gz_
                    target[h * M + u * 16 : h * M + u * 16 + 16, c * PT : (c + 1) * PT] = value.astype(BF)

    def pair(u, carry, with_far):
        for t in (2 * u, 2 * u + 1):
            near_copy(block_of(t)).wait_recv()
            z_copy(0, block_of(t)).wait_recv()
            z_copy(1, block_of(t)).wait_recv()
            if with_far:
                far_copy(t - 4).wait_recv()
        if not with_far:

            @pl.when(u == 0)
            def _():
                far_copy(2).start()
                far_copy(3).start()

        for b in range(2):
            t = 2 * u + b
            before = block_of(lax.rem(t + 7, 8))

            def first(t=t, b=b, before=before):
                prepare(t, b, with_far)
                dot(7, 1, turned[before])

            run(first, lambda t=t: turned[block_of(t)], functools.partial(terms, b))
        return carry

    lax.fori_loop(0, 2, functools.partial(pair, with_far=False), 0)
    lax.fori_loop(2, 4, functools.partial(pair, with_far=True), 0)

    weight_copy.wait_recv()
    foreign = swfar[...]
    foreign = jnp.where(odd == 1, pltpu.roll(foreign, LV // 2, 1), foreign)

    def prepare_cross(v):
        wide = [weighted_columns(foreign, v * 32 + 16 * h, 16) for h in range(2)]
        pk = []
        for h in range(2):
            mine = 2 * v + h + 4 * odd
            for c in range(3):
                here = far[2 * v + h, c]
                if c == 0:
                    pk.append(jnp.dot(self_[...], here.T, preferred_element_type=F32).astype(BF))
                at = c * PT + h * CH
                cross_tested[v, :, at : at + CH] = (here.astype(F32) * wide[h]).astype(BF).T
                grads[v][c, :, h * CH : (h + 1) * CH] = planes[c, 0, rows_of(mine), :].T.astype(F32)
            for j in range(JW):
                picks[v][j, :, h * CH : (h + 1) * CH] = jnp.broadcast_to(
                    pk[h][j : j + 1].astype(F32), (8, CH)
                )

    def cross_terms(v, step, target):
        scale = []
        for h in range(2):
            p = picks[v][2 * step + h].astype(BF)
            scale.append(jnp.concatenate([p, p], axis=0))
        for c in range(3):
            for u in range(8):
                tile = grads[v][c, u * 16 : u * 16 + 16, :].astype(BF)
                for h in range(2):
                    target[h * M + u * 16 : h * M + u * 16 + 16, c * PT : (c + 1) * PT] = scale[h] * tile

    for v in range(2):

        def first(v=v):
            prepare_cross(v)
            dot(7, 1, turned[block_of(7)] if v == 0 else cross_tested[0])

        run(first, lambda v=v: cross_tested[v], functools.partial(cross_terms, v))
    dot(7, 1, cross_tested[1])

    finish = reduce_parts(total, out, *reduction)
    for k in range(8):
        near_copy(k).wait_send()
        z_copy(0, k).wait_send()
        z_copy(1, k).wait_send()
        if k < 4:
            far_copy(k).wait_send()
    weight_copy.wait_send()
    finish()


VM = pl.BlockSpec(memory_space=pltpu.VMEM)
SM = pl.BlockSpec(memory_space=pltpu.SMEM)
HB = pl.BlockSpec(memory_space=pl.ANY)


def local(modes, weights, counts, mode_index):
    return pl.pallas_call(
        local_kernel,
        out_shape=jax.ShapeDtypeStruct((JW, 4, M), F32),
        in_specs=[HB, HB, SM, SM],
        out_specs=VM,
        scratch_shapes=[
            pltpu.VMEM((2, CZ, LV), F32),
            pltpu.VMEM((M, JW * M), F32),
            pltpu.VMEM((3, 2, ROWS + 2 * PAD, M), BF),
            pltpu.VMEM((8, 3, CH, M), BF),
            pltpu.VMEM((4, 3, CH, M), BF),
            pltpu.VMEM((2, 8, 96, M), BF),
            pltpu.VMEM((2, 8, 96, M), BF),
            pltpu.VMEM((2, CZ, LV), F32),
            pltpu.VMEM((CZ, LV), F32),
            pltpu.VMEM((8, M, 3 * PT), BF),
            pltpu.VMEM((2, M, 3 * PT), BF),
            [pltpu.VMEM((9, M, PT), F32)] * 2,
            [pltpu.VMEM((3 * JW, 8, PT), F32)] * 2,
            [pltpu.VMEM((2 * M, 3 * PT), BF)] * 2,
            pltpu.VMEM((PT, PT), BF),
            pltpu.VMEM((3 * JW, 3 * M), BF),
            pltpu.VMEM((JW, M), BF),
            pltpu.SemaphoreType.DMA((7,)),
            pltpu.SemaphoreType.DMA((8,)),
            pltpu.SemaphoreType.DMA((8,)),
            pltpu.SemaphoreType.DMA((4,)),
            pltpu.SemaphoreType.DMA((4,)),
            pltpu.SemaphoreType.DMA((2, 8)),
            pltpu.SemaphoreType.DMA((2, 8)),
            pltpu.SemaphoreType.DMA((2,)),
            pltpu.VMEM((16, 8, JW * M), F32),
            pltpu.VMEM((16, 8, 8 * M), F32),
            pltpu.VMEM((16, 8, 8 * M), BF),
            pltpu.VMEM((16, 8, 8 * M), BF),
            pltpu.VMEM((2, 4, 8 * M), F32),
            pltpu.VMEM((8, 4, 8 * M), F32),
            pltpu.VMEM((JW, 4, M), F32),
            pltpu.SemaphoreType.DMA((4,)),
            pltpu.SemaphoreType.DMA((4,)),
            pltpu.SemaphoreType.DMA((16,)),
            pltpu.SemaphoreType.DMA((16,)),
            pltpu.SemaphoreType.DMA((8,)),
            pltpu.SemaphoreType.DMA((8,)),
            pltpu.SemaphoreType.DMA((2,)),
        ],
        compiler_params=pltpu.CompilerParams(
            vmem_limit_bytes=67043328, collective_id=0, has_side_effects=True
        ),
    )(modes.reshape(3, 2, ROWS, M), jnp.swapaxes(weights, 1, 2), counts, mode_index)


def solution(mesh):
    placed = (P(None, "gx", None, "gz", None), P("gx", None, "gz"), P(("gx", "gz")), P())
    return jax.shard_map(
        local, mesh=mesh, in_specs=placed, out_specs=P(None, "gz", None), check_vma=False
    )
```

```python
import functools

import jax
import jax.numpy as jnp
from jax import lax
from jax.experimental import pallas as pl
from jax.experimental.pallas import tpu as pltpu
from jax.sharding import PartitionSpec as P

MESH = pl.DeviceIdType.MESH
BF = jnp.bfloat16
F32 = jnp.float32
M = 128
JW = 16
LV = 128
CZ = 8
ROWS = LV * CZ
PAD = 16
CH = 128
PT = 2 * CH
HALF = ROWS // 2


def iota(shape, dim):
    return lax.broadcasted_iota(jnp.int32, shape, dim)


def pick_rows(idx_ref, scales):
    count = len(scales) * JW
    row, col = iota((count, M), 0), iota((count, M), 1)
    wanted = jnp.zeros((count, M), jnp.int32)
    for j in range(JW):
        wanted = jnp.where(row % JW == j, idx_ref[j], wanted)
    blocks = [
        jnp.where((col == wanted) & (row // JW == d), scale, 0.0).astype(BF)
        for d, scale in enumerate(scales)
    ]
    return jnp.concatenate(blocks, axis=1)


def weighted_columns(sw, first, levels):
    return jnp.concatenate(
        [jnp.broadcast_to(sw[:, y : y + 1], (CZ, M)) for y in range(first, first + levels)], axis=0
    )


def stencil_matrix():
    row, col = iota((PT, PT), 0), iota((PT, PT), 1)
    point = lax.rem(col, CH)
    lev, z = point // CZ, lax.rem(point, CZ)
    up = jnp.where(point + CZ < CH, point + CZ, point + CZ + 16)
    down = jnp.where(point >= CZ, point - CZ, CH + 8 + point)
    ahead = jnp.where(z < CZ - 1, point + 1, CH + 48 + lev)
    behind = jnp.where(z > 0, point - 1, CH + 32 + lev)
    plus = jnp.where(col < CH, up, ahead)
    minus = jnp.where(col < CH, down, behind)
    return (jnp.where(row == plus, 1.0, 0.0) - jnp.where(row == minus, 1.0, 0.0)).astype(BF)


def select_rows():
    row, col = iota((32, CH), 0), iota((32, CH), 1)
    return jnp.where(col == lax.rem(row, 16) * CZ + (row // 16) * (CZ - 1), 1.0, 0.0).astype(BF)


def place():
    gx, gz = lax.axis_index("gx"), lax.axis_index("gz")
    core, zh = lax.rem(gx, 2), gx // 2
    x, low, y = gz // 8, lax.rem(gz // 4, 2), lax.rem(gz, 4)
    return gx, gz, core, x, low, y, x * 4 + y, zh * 2 + low


def plane_peer(p):
    gx, _, _, _, low, _, _, _ = place()
    return (gx, (p // 4) * 8 + low * 4 + lax.rem(p, 4))


def column_peer(p):
    _, _, core, x, _, y, _, _ = place()
    return ((p // 2) * 2 + core, x * 8 + lax.rem(p, 2) * 4 + y)


def reduction_peers():
    _, _, _, _, _, _, q, z = place()
    return [plane_peer(lax.rem(q + d, 16)) for d in range(1, 16)] + [
        column_peer(lax.rem(z + d, 8)) for d in range(1, 8)
    ]


def reduce_parts(
    total, out, part, pair, send, got, column, stack, whole, asend, arecv, bsend, brecv, csend, crecv, dsem
):
    gx, gz, core, x, low, y, q, z = place()
    partner = (gx + 1 - 2 * core, gz)

    width = 8 * M
    own = pl.ds(pl.multiple_of(core * width, width), width)
    theirs = pl.ds(pl.multiple_of((1 - core) * width, width), width)

    def pair_copy(g):
        quarter = pl.ds(g * 4, 4)
        return pltpu.make_async_remote_copy(
            src_ref=part.at[quarter, :, theirs],
            dst_ref=pair.at[quarter],
            send_sem=asend.at[g],
            recv_sem=arecv.at[g],
            device_id=partner,
            device_id_type=MESH,
        )

    def plane_copy(dest, slot):
        return pltpu.make_async_remote_copy(
            src_ref=send.at[dest],
            dst_ref=got.at[slot],
            send_sem=bsend.at[dest],
            recv_sem=brecv.at[slot],
            device_id=plane_peer(dest),
            device_id_type=MESH,
        )

    def column_copy(dest, slot):
        return pltpu.make_async_remote_copy(
            src_ref=column.at[lax.rem(dest, 2)],
            dst_ref=stack.at[slot],
            send_sem=csend.at[dest],
            recv_sem=crecv.at[slot],
            device_id=column_peer(dest),
            device_id_type=MESH,
        )

    for g in range(4):
        for b in range(g * 4, g * 4 + 4):
            for half in range(2):
                owner = (b // 4) * 8 + half * 4 + b % 4
                part[b, half * 4 : half * 4 + 4, :] = total[owner * 4 : owner * 4 + 4, :]
        pair_copy(g).start()
    for g in range(4):
        pair_copy(g).wait_recv()
        for b in range(g * 4, g * 4 + 4):
            send[b] = (part[b, :, own] + pair[b]).astype(BF)

            @pl.when(b != q)
            def _(b=b):
                plane_copy(b, q).start()

    mine = send[q].astype(F32)
    for d in range(1, 16):
        p = lax.rem(q + d, 16)
        plane_copy(p, p).wait_recv()
        mine = mine + got[p].astype(F32)
    column[0] = mine[:4]
    column[1] = mine[4:]
    for d in (4, 3, 5, 2, 6, 1, 7):
        column_copy(lax.rem(z + d, 8), z).start()
    stack[z] = column[low]
    for d in range(1, 8):
        p = lax.rem(z + d, 8)
        column_copy(p, p).wait_recv()
    mine = stack[0]
    for p in range(1, 8):
        mine = mine + stack[p]
    for j in range(8):
        whole[core * 8 + j] = mine[:, j * M : (j + 1) * M]
    block = whole.at[pl.ds(core * 8, 8)]
    last = pltpu.make_async_remote_copy(
        src_ref=block, dst_ref=block, send_sem=dsem.at[0], recv_sem=dsem.at[1],
        device_id=partner, device_id_type=MESH,
    )
    last.start()
    last.wait_recv()
    out[...] = whole[...]

    def finish():
        for g in range(4):
            pair_copy(g).wait_send()
        for d in range(1, 16):
            plane_copy(lax.rem(q + d, 16), q).wait_send()
        for d in range(1, 8):
            column_copy(lax.rem(z + d, 8), z).wait_send()
        last.wait_send()

    return finish


def local_kernel(
    modes, weights, counts, idx, out,
    weights_in, total, planes, near, far, zsend, zgot, sw, swfar, turned, cross_tested, grads, picks, spread, stencil, sel, self_,
    local_sem, near_s, near_r, far_s, far_r, z_s, z_r, w_sem, *reduction,
):
    gx, gz = lax.axis_index("gx"), lax.axis_index("gz")
    odd = lax.rem(gx, 2)
    sign = jnp.where(odd == 0, 0.5, -0.5).astype(F32)
    near_peer = (gx + 1 - 2 * odd, gz)
    far_peer = (lax.rem(gx + 7 + 2 * odd, 8), gz)
    z_peers = ((gx, lax.rem(gz + 31, 32)), (gx, lax.rem(gz + 1, 32)))

    barrier = pltpu.get_barrier_semaphore()
    peers = [near_peer, far_peer, *z_peers, *reduction_peers()]
    for peer in peers:
        pl.semaphore_signal(barrier, inc=1, device_id=peer, device_id_type=MESH)
    small = [pltpu.make_async_copy(weights, weights_in, local_sem.at[6])]
    copies = []
    for c in range(3):
        for side in range(2):
            which = odd if side == 0 else 1 - odd
            copies.append(
                pltpu.make_async_copy(
                    modes.at[c, which], planes.at[c, side, pl.ds(PAD, ROWS)], local_sem.at[2 * c + side]
                )
            )
    for copy in (*small, *copies):
        copy.start()
    for c in range(3):
        for side in range(2):
            planes[c, side, pl.ds(0, PAD), :] = jnp.zeros((PAD, M), BF)
            planes[c, side, pl.ds(PAD + ROWS, PAD), :] = jnp.zeros((PAD, M), BF)
    for copy in small:
        copy.wait()
    for side in range(2):
        which = odd if side == 0 else 1 - odd
        w = weights_in[which]
        sw[side] = jnp.where(iota((CZ, LV), 1) < counts[0], w, jnp.zeros_like(w))
    stencil[...] = stencil_matrix()
    sel[...] = pick_rows(idx, (sign, 0.5, 0.5))
    self_[...] = pick_rows(idx, (sign,))
    total[...] = jnp.zeros_like(total)
    spread[3][...] = jnp.zeros_like(spread[3])
    ends = select_rows()
    for copy in copies:
        copy.wait()

    def block_of(t):
        return lax.rem(t + 4 * (1 - odd), 8)

    def rows_of(k):
        return pl.ds(pl.multiple_of(PAD + k * CH, 16), CH)

    def near_copy(k):
        return pltpu.make_async_remote_copy(
            src_ref=planes.at[:, 1, rows_of(k)], dst_ref=near.at[k],
            send_sem=near_s.at[k], recv_sem=near_r.at[k], device_id=near_peer, device_id_type=MESH,
        )

    def far_copy(p):
        return pltpu.make_async_remote_copy(
            src_ref=planes.at[:, 0, rows_of(p + 4 * (1 - odd))], dst_ref=far.at[p],
            send_sem=far_s.at[p], recv_sem=far_r.at[p], device_id=far_peer, device_id_type=MESH,
        )

    def z_copy(direction, k):
        return pltpu.make_async_remote_copy(
            src_ref=zsend.at[direction, k], dst_ref=zgot.at[direction, k],
            send_sem=z_s.at[direction, k], recv_sem=z_r.at[direction, k],
            device_id=z_peers[direction], device_id_type=MESH,
        )

    weight_copy = pltpu.make_async_remote_copy(
        src_ref=sw.at[0], dst_ref=swfar, send_sem=w_sem.at[0], recv_sem=w_sem.at[1],
        device_id=far_peer, device_id_type=MESH,
    )

    def send_edges(t, carry):
        k = block_of(t)
        for c in range(3):
            for side in range(2):
                edge = jnp.dot(ends, planes[c, side, rows_of(k), :], preferred_element_type=F32).astype(BF)
                at = (2 * c + side) * 16
                zsend[0, k, at : at + 16, :] = edge[:16]
                zsend[1, k, at : at + 16, :] = edge[16:]
        return carry

    lax.fori_loop(0, 8, send_edges, 0)
    pl.semaphore_wait(barrier, len(peers))
    for t in range(8):
        near_copy(lax.rem(t + 4 * odd, 8)).start()
        z_copy(0, block_of(t)).start()
        z_copy(1, block_of(t)).start()
    weight_copy.start()
    for k in range(8):
        for side in range(2):
            wide = weighted_columns(sw[side], k * 16, 16)
            for c in range(3):
                here = planes[c, side, PAD + k * CH : PAD + (k + 1) * CH, :].astype(F32)
                at = c * PT + side * CH
                turned[k, :, at : at + CH] = (here * wide).astype(BF).T

    far_copy(0).start()
    far_copy(1).start()

    def dot(step, buffer, tested):
        cols = slice(step * 256, step * 256 + 256)
        total[:, cols] += lax.dot_general(
            tested, spread[buffer][...], (((1,), (1,)), ((), ())), preferred_element_type=F32
        )

    def run(first, tested, terms):
        first()
        terms(0, spread[0])
        for step in range(7):
            dot(step, step % 4, tested())
            terms(step + 1, spread[(step + 1) % 4])

    def prepare(t, b, with_far):
        k = block_of(t)
        g = grads[b]
        flipped = [[], []]
        for side in range(2):
            lanes = slice(side * CH, (side + 1) * CH)
            for c in range(3):
                at = (2 * c + side) * 16
                stacked = jnp.concatenate(
                    [
                        planes[c, side, rows_of(k), :],
                        planes[c, side, pl.ds(pl.multiple_of(k * CH, 16), 16), :],
                        planes[c, side, pl.ds(pl.multiple_of(PAD + (k + 1) * CH, 16), 16), :],
                        zgot[1, k, at : at + 16, :],
                        zgot[0, k, at : at + 16, :],
                        jnp.zeros((64, M), BF),
                    ],
                    axis=0,
                ).T
                both = jnp.dot(stacked, stencil[...], preferred_element_type=F32)
                g[3 + c, :, lanes] = both[:, :CH]
                g[6 + c, :, lanes] = both[:, CH:]
                flipped[side].append(stacked[:, :CH])
            pk = jnp.dot(sel[...], jnp.concatenate(flipped[side], axis=0), preferred_element_type=F32)
            for r in range(3 * JW):
                picks[b][r, :, lanes] = jnp.broadcast_to(pk[r : r + 1], (8, CH))
        for c in range(3):
            inner = flipped[1][c].astype(F32)
            if with_far:
                inner = inner - far[t - 4, c].T.astype(F32)
            g[c, :, :CH] = inner
            g[c, :, CH:] = near[k, c].T.astype(F32) - flipped[0][c].astype(F32)

    def terms(b, step, target):
        g, pk = grads[b], picks[b]
        scale = []
        for h in range(2):
            p = [pk[d * JW + 2 * step + h] for d in range(3)]
            scale.append([jnp.concatenate([v, v], axis=0) for v in p])
        for c in range(3):
            for u in range(8):
                tile = slice(u * 16, u * 16 + 16)
                gx_, gy_, gz_ = g[c, tile, :], g[3 + c, tile, :], g[6 + c, tile, :]
                for h in range(2):
                    px, py, pz = scale[h]
                    value = px * gx_ + py * gy_ + pz * gz_
                    target[h * M + u * 16 : h * M + u * 16 + 16, c * PT : (c + 1) * PT] = value.astype(BF)

    def pair(u, carry, with_far):
        for t in (2 * u, 2 * u + 1):
            near_copy(block_of(t)).wait_recv()
            z_copy(0, block_of(t)).wait_recv()
            z_copy(1, block_of(t)).wait_recv()
            if with_far:
                far_copy(t - 4).wait_recv()
        if not with_far:

            @pl.when(u == 0)
            def _():
                far_copy(2).start()
                far_copy(3).start()

        for b in range(2):
            t = 2 * u + b
            before = block_of(lax.rem(t + 7, 8))

            def first(t=t, b=b, before=before):
                prepare(t, b, with_far)
                dot(7, 3, turned[before])

            run(first, lambda t=t: turned[block_of(t)], functools.partial(terms, b))
        return carry

    lax.fori_loop(0, 2, functools.partial(pair, with_far=False), 0)
    lax.fori_loop(2, 4, functools.partial(pair, with_far=True), 0)

    weight_copy.wait_recv()
    foreign = swfar[...]
    foreign = jnp.where(odd == 1, pltpu.roll(foreign, LV // 2, 1), foreign)

    def prepare_cross(v):
        wide = [weighted_columns(foreign, v * 32 + 16 * h, 16) for h in range(2)]
        pk = []
        for h in range(2):
            mine = 2 * v + h + 4 * odd
            for c in range(3):
                here = far[2 * v + h, c]
                if c == 0:
                    pk.append(jnp.dot(self_[...], here.T, preferred_element_type=F32).astype(BF))
                at = c * PT + h * CH
                cross_tested[v, :, at : at + CH] = (here.astype(F32) * wide[h]).astype(BF).T
                grads[v][c, :, h * CH : (h + 1) * CH] = planes[c, 0, rows_of(mine), :].T.astype(F32)
            for j in range(JW):
                picks[v][j, :, h * CH : (h + 1) * CH] = jnp.broadcast_to(
                    pk[h][j : j + 1].astype(F32), (8, CH)
                )

    def cross_terms(v, step, target):
        scale = []
        for h in range(2):
            p = picks[v][2 * step + h].astype(BF)
            scale.append(jnp.concatenate([p, p], axis=0))
        for c in range(3):
            for u in range(8):
                tile = grads[v][c, u * 16 : u * 16 + 16, :].astype(BF)
                for h in range(2):
                    target[h * M + u * 16 : h * M + u * 16 + 16, c * PT : (c + 1) * PT] = scale[h] * tile

    for v in range(2):

        def first(v=v):
            prepare_cross(v)
            dot(7, 3, turned[block_of(7)] if v == 0 else cross_tested[0])

        run(first, lambda v=v: cross_tested[v], functools.partial(cross_terms, v))
    dot(7, 3, cross_tested[1])

    finish = reduce_parts(total, out, *reduction)
    for k in range(8):
        near_copy(k).wait_send()
        z_copy(0, k).wait_send()
        z_copy(1, k).wait_send()
        if k < 4:
            far_copy(k).wait_send()
    weight_copy.wait_send()
    finish()


VM = pl.BlockSpec(memory_space=pltpu.VMEM)
SM = pl.BlockSpec(memory_space=pltpu.SMEM)
HB = pl.BlockSpec(memory_space=pl.ANY)


def local(modes, weights, counts, mode_index):
    return pl.pallas_call(
        local_kernel,
        out_shape=jax.ShapeDtypeStruct((JW, 4, M), F32),
        in_specs=[HB, HB, SM, SM],
        out_specs=VM,
        scratch_shapes=[
            pltpu.VMEM((2, CZ, LV), F32),
            pltpu.VMEM((M, JW * M), F32),
            pltpu.VMEM((3, 2, ROWS + 2 * PAD, M), BF),
            pltpu.VMEM((8, 3, CH, M), BF),
            pltpu.VMEM((4, 3, CH, M), BF),
            pltpu.VMEM((2, 8, 96, M), BF),
            pltpu.VMEM((2, 8, 96, M), BF),
            pltpu.VMEM((2, CZ, LV), F32),
            pltpu.VMEM((CZ, LV), F32),
            pltpu.VMEM((8, M, 3 * PT), BF),
            pltpu.VMEM((2, M, 3 * PT), BF),
            [pltpu.VMEM((9, M, PT), F32)] * 2,
            [pltpu.VMEM((3 * JW, 8, PT), F32)] * 2,
            [pltpu.VMEM((2 * M, 3 * PT), BF)] * 4,
            pltpu.VMEM((PT, PT), BF),
            pltpu.VMEM((3 * JW, 3 * M), BF),
            pltpu.VMEM((JW, M), BF),
            pltpu.SemaphoreType.DMA((7,)),
            pltpu.SemaphoreType.DMA((8,)),
            pltpu.SemaphoreType.DMA((8,)),
            pltpu.SemaphoreType.DMA((4,)),
            pltpu.SemaphoreType.DMA((4,)),
            pltpu.SemaphoreType.DMA((2, 8)),
            pltpu.SemaphoreType.DMA((2, 8)),
            pltpu.SemaphoreType.DMA((2,)),
            pltpu.VMEM((16, 8, JW * M), F32),
            pltpu.VMEM((16, 8, 8 * M), F32),
            pltpu.VMEM((16, 8, 8 * M), BF),
            pltpu.VMEM((16, 8, 8 * M), BF),
            pltpu.VMEM((2, 4, 8 * M), F32),
            pltpu.VMEM((8, 4, 8 * M), F32),
            pltpu.VMEM((JW, 4, M), F32),
            pltpu.SemaphoreType.DMA((4,)),
            pltpu.SemaphoreType.DMA((4,)),
            pltpu.SemaphoreType.DMA((16,)),
            pltpu.SemaphoreType.DMA((16,)),
            pltpu.SemaphoreType.DMA((8,)),
            pltpu.SemaphoreType.DMA((8,)),
            pltpu.SemaphoreType.DMA((2,)),
        ],
        compiler_params=pltpu.CompilerParams(
            vmem_limit_bytes=67043328, collective_id=0, has_side_effects=True
        ),
    )(modes.reshape(3, 2, ROWS, M), jnp.swapaxes(weights, 1, 2), counts, mode_index)


def solution(mesh):
    placed = (P(None, "gx", None, "gz", None), P("gx", None, "gz"), P(("gx", "gz")), P())
    return jax.shard_map(
        local, mesh=mesh, in_specs=placed, out_specs=P(None, "gz", None), check_vma=False
    )
```

```python
import functools

import jax
import jax.numpy as jnp
from jax import lax
from jax.experimental import pallas as pl
from jax.experimental.pallas import tpu as pltpu
from jax.sharding import PartitionSpec as P

MESH = pl.DeviceIdType.MESH
BF = jnp.bfloat16
F32 = jnp.float32
M = 128
JW = 16
LV = 128
CZ = 8
ROWS = LV * CZ
PAD = 16
CH = 128
PT = 2 * CH
HALF = ROWS // 2


def iota(shape, dim):
    return lax.broadcasted_iota(jnp.int32, shape, dim)


def pick_rows(idx_ref, scales):
    count = len(scales) * JW
    row, col = iota((count, M), 0), iota((count, M), 1)
    wanted = jnp.zeros((count, M), jnp.int32)
    for j in range(JW):
        wanted = jnp.where(row % JW == j, idx_ref[j], wanted)
    blocks = [
        jnp.where((col == wanted) & (row // JW == d), scale, 0.0).astype(BF)
        for d, scale in enumerate(scales)
    ]
    return jnp.concatenate(blocks, axis=1)


def weighted_columns(sw, first, levels):
    return jnp.concatenate(
        [jnp.broadcast_to(sw[:, y : y + 1], (CZ, M)) for y in range(first, first + levels)], axis=0
    )


def stencil_matrix():
    row, col = iota((PT, PT), 0), iota((PT, PT), 1)
    point = lax.rem(col, CH)
    lev, z = point // CZ, lax.rem(point, CZ)
    up = jnp.where(point + CZ < CH, point + CZ, point + CZ + 16)
    down = jnp.where(point >= CZ, point - CZ, CH + 8 + point)
    ahead = jnp.where(z < CZ - 1, point + 1, CH + 48 + lev)
    behind = jnp.where(z > 0, point - 1, CH + 32 + lev)
    plus = jnp.where(col < CH, up, ahead)
    minus = jnp.where(col < CH, down, behind)
    return (jnp.where(row == plus, 1.0, 0.0) - jnp.where(row == minus, 1.0, 0.0)).astype(BF)


def select_rows():
    row, col = iota((32, CH), 0), iota((32, CH), 1)
    return jnp.where(col == lax.rem(row, 16) * CZ + (row // 16) * (CZ - 1), 1.0, 0.0).astype(BF)


def place():
    gx, gz = lax.axis_index("gx"), lax.axis_index("gz")
    core, zh = lax.rem(gx, 2), gx // 2
    x, low, y = gz // 8, lax.rem(gz // 4, 2), lax.rem(gz, 4)
    return gx, gz, core, x, low, y, x * 4 + y, zh * 2 + low


def plane_peer(p):
    gx, _, _, _, low, _, _, _ = place()
    return (gx, (p // 4) * 8 + low * 4 + lax.rem(p, 4))


def column_peer(p):
    _, _, core, x, _, y, _, _ = place()
    return ((p // 2) * 2 + core, x * 8 + lax.rem(p, 2) * 4 + y)


def reduction_peers():
    _, _, _, _, _, _, q, z = place()
    return [plane_peer(lax.rem(q + d, 16)) for d in range(1, 16)] + [
        column_peer(lax.rem(z + d, 8)) for d in range(1, 8)
    ]


def reduce_parts(
    total, out, part, pair, send, got, column, stack, whole, asend, arecv, bsend, brecv, csend, crecv, dsem
):
    gx, gz, core, x, low, y, q, z = place()
    partner = (gx + 1 - 2 * core, gz)

    width = 8 * M
    own = pl.ds(pl.multiple_of(core * width, width), width)
    theirs = pl.ds(pl.multiple_of((1 - core) * width, width), width)

    def pair_copy(g):
        quarter = pl.ds(g * 4, 4)
        return pltpu.make_async_remote_copy(
            src_ref=part.at[quarter, :, theirs],
            dst_ref=pair.at[quarter],
            send_sem=asend.at[g],
            recv_sem=arecv.at[g],
            device_id=partner,
            device_id_type=MESH,
        )

    def plane_copy(dest, slot):
        return pltpu.make_async_remote_copy(
            src_ref=send.at[dest],
            dst_ref=got.at[slot],
            send_sem=bsend.at[dest],
            recv_sem=brecv.at[slot],
            device_id=plane_peer(dest),
            device_id_type=MESH,
        )

    def column_copy(dest, slot):
        return pltpu.make_async_remote_copy(
            src_ref=column.at[lax.rem(dest, 2)],
            dst_ref=stack.at[slot],
            send_sem=csend.at[dest],
            recv_sem=crecv.at[slot],
            device_id=column_peer(dest),
            device_id_type=MESH,
        )

    for g in range(4):
        for b in range(g * 4, g * 4 + 4):
            for half in range(2):
                owner = (b // 4) * 8 + half * 4 + b % 4
                part[b, half * 4 : half * 4 + 4, :] = total[owner * 4 : owner * 4 + 4, :]
        pair_copy(g).start()
    for g in range(4):
        pair_copy(g).wait_recv()
        for b in range(g * 4, g * 4 + 4):
            send[b] = (part[b, :, own] + pair[b]).astype(BF)

            @pl.when(b != q)
            def _(b=b):
                plane_copy(b, q).start()

    mine = send[q].astype(F32)
    for d in range(1, 16):
        p = lax.rem(q + d, 16)
        plane_copy(p, p).wait_recv()
        mine = mine + got[p].astype(F32)
    column[0] = mine[:4]
    column[1] = mine[4:]
    for d in (4, 3, 5, 2, 6, 1, 7):
        column_copy(lax.rem(z + d, 8), z).start()
    stack[z] = column[low]
    for d in range(1, 8):
        p = lax.rem(z + d, 8)
        column_copy(p, p).wait_recv()
    mine = stack[0]
    for p in range(1, 8):
        mine = mine + stack[p]
    for j in range(8):
        whole[core * 8 + j] = mine[:, j * M : (j + 1) * M]
    block = whole.at[pl.ds(core * 8, 8)]
    last = pltpu.make_async_remote_copy(
        src_ref=block, dst_ref=block, send_sem=dsem.at[0], recv_sem=dsem.at[1],
        device_id=partner, device_id_type=MESH,
    )
    last.start()
    last.wait_recv()
    out[...] = whole[...]

    def finish():
        for g in range(4):
            pair_copy(g).wait_send()
        for d in range(1, 16):
            plane_copy(lax.rem(q + d, 16), q).wait_send()
        for d in range(1, 8):
            column_copy(lax.rem(z + d, 8), z).wait_send()
        last.wait_send()

    return finish


def local_kernel(
    modes, weights, counts, idx, out,
    weights_in, total, planes, near, far, zsend, zgot, sw, swfar, turned, cross_tested, grads, picks, spread, stencil, sel, self_,
    local_sem, near_s, near_r, far_s, far_r, z_s, z_r, w_sem, *reduction,
):
    gx, gz = lax.axis_index("gx"), lax.axis_index("gz")
    odd = lax.rem(gx, 2)
    sign = jnp.where(odd == 0, 0.5, -0.5).astype(F32)
    near_peer = (gx + 1 - 2 * odd, gz)
    far_peer = (lax.rem(gx + 7 + 2 * odd, 8), gz)
    z_peers = ((gx, lax.rem(gz + 31, 32)), (gx, lax.rem(gz + 1, 32)))

    barrier = pltpu.get_barrier_semaphore()
    peers = [near_peer, far_peer, *z_peers, *reduction_peers()]
    for peer in peers:
        pl.semaphore_signal(barrier, inc=1, device_id=peer, device_id_type=MESH)
    small = [pltpu.make_async_copy(weights, weights_in, local_sem.at[6])]
    copies = []
    for c in range(3):
        for side in range(2):
            which = odd if side == 0 else 1 - odd
            copies.append(
                pltpu.make_async_copy(
                    modes.at[c, which], planes.at[c, side, pl.ds(PAD, ROWS)], local_sem.at[2 * c + side]
                )
            )
    for copy in (*small, *copies):
        copy.start()
    for c in range(3):
        for side in range(2):
            planes[c, side, pl.ds(0, PAD), :] = jnp.zeros((PAD, M), BF)
            planes[c, side, pl.ds(PAD + ROWS, PAD), :] = jnp.zeros((PAD, M), BF)
    for copy in small:
        copy.wait()
    for side in range(2):
        which = odd if side == 0 else 1 - odd
        w = weights_in[which]
        sw[side] = jnp.where(iota((CZ, LV), 1) < counts[0], w, jnp.zeros_like(w))
    stencil[...] = stencil_matrix()
    sel[...] = pick_rows(idx, (sign, 0.5, 0.5))
    self_[...] = pick_rows(idx, (sign,))
    ends = select_rows()
    for copy in copies:
        copy.wait()

    def block_of(t):
        return lax.rem(t + 4 * (1 - odd), 8)

    def rows_of(k):
        return pl.ds(pl.multiple_of(PAD + k * CH, 16), CH)

    def near_copy(k):
        return pltpu.make_async_remote_copy(
            src_ref=planes.at[:, 1, rows_of(k)], dst_ref=near.at[k],
            send_sem=near_s.at[k], recv_sem=near_r.at[k], device_id=near_peer, device_id_type=MESH,
        )

    def far_copy(p):
        return pltpu.make_async_remote_copy(
            src_ref=planes.at[:, 0, rows_of(p + 4 * (1 - odd))], dst_ref=far.at[p],
            send_sem=far_s.at[p], recv_sem=far_r.at[p], device_id=far_peer, device_id_type=MESH,
        )

    def z_copy(direction, k):
        return pltpu.make_async_remote_copy(
            src_ref=zsend.at[direction, k], dst_ref=zgot.at[direction, k],
            send_sem=z_s.at[direction, k], recv_sem=z_r.at[direction, k],
            device_id=z_peers[direction], device_id_type=MESH,
        )

    weight_copy = pltpu.make_async_remote_copy(
        src_ref=sw.at[0], dst_ref=swfar, send_sem=w_sem.at[0], recv_sem=w_sem.at[1],
        device_id=far_peer, device_id_type=MESH,
    )

    def send_edges(t, carry):
        k = block_of(t)
        for c in range(3):
            for side in range(2):
                edge = jnp.dot(ends, planes[c, side, rows_of(k), :], preferred_element_type=F32).astype(BF)
                at = (2 * c + side) * 16
                zsend[0, k, at : at + 16, :] = edge[:16]
                zsend[1, k, at : at + 16, :] = edge[16:]
        return carry

    lax.fori_loop(0, 8, send_edges, 0)
    pl.semaphore_wait(barrier, len(peers))
    for t in range(8):
        near_copy(lax.rem(t + 4 * odd, 8)).start()
        z_copy(0, block_of(t)).start()
        z_copy(1, block_of(t)).start()
    for p in range(4):
        far_copy(p).start()
    weight_copy.start()
    for k in range(8):
        for side in range(2):
            wide = weighted_columns(sw[side], k * 16, 16)
            for c in range(3):
                here = planes[c, side, PAD + k * CH : PAD + (k + 1) * CH, :].astype(F32)
                at = c * PT + side * CH
                turned[k, :, at : at + CH] = (here * wide).astype(BF).T

    def prepare(t):
        k, b, with_far = block_of(t), t % 2, t >= 4
        near_copy(k).wait_recv()
        z_copy(0, k).wait_recv()
        z_copy(1, k).wait_recv()
        if with_far:
            far_copy(t - 4).wait_recv()
        g = grads[b]
        flipped = [[], []]
        for side in range(2):
            lanes = slice(side * CH, (side + 1) * CH)
            for c in range(3):
                at = (2 * c + side) * 16
                stacked = jnp.concatenate(
                    [
                        planes[c, side, rows_of(k), :],
                        planes[c, side, pl.ds(pl.multiple_of(k * CH, 16), 16), :],
                        planes[c, side, pl.ds(pl.multiple_of(PAD + (k + 1) * CH, 16), 16), :],
                        zgot[1, k, at : at + 16, :],
                        zgot[0, k, at : at + 16, :],
                        jnp.zeros((64, M), BF),
                    ],
                    axis=0,
                ).T
                both = jnp.dot(stacked, stencil[...], preferred_element_type=F32)
                g[3 + c, :, lanes] = both[:, :CH]
                g[6 + c, :, lanes] = both[:, CH:]
                flipped[side].append(stacked[:, :CH])
            pk = jnp.dot(sel[...], jnp.concatenate(flipped[side], axis=0), preferred_element_type=F32)
            for r in range(3 * JW):
                picks[b][r, :, lanes] = jnp.broadcast_to(pk[r : r + 1], (8, CH))
        for c in range(3):
            inner = flipped[1][c].astype(F32)
            if with_far:
                inner = inner - far[t - 4, c].T.astype(F32)
            g[c, :, :CH] = inner
            g[c, :, CH:] = near[k, c].T.astype(F32) - flipped[0][c].astype(F32)

    def terms(b, step, target):
        g, pk = grads[b], picks[b]
        scale = []
        for h in range(2):
            p = [pk[d * JW + 2 * step + h] for d in range(3)]
            scale.append([jnp.concatenate([v, v], axis=0) for v in p])
        for c in range(3):
            for u in range(8):
                tile = slice(u * 16, u * 16 + 16)
                gx_, gy_, gz_ = g[c, tile, :], g[3 + c, tile, :], g[6 + c, tile, :]
                for h in range(2):
                    px, py, pz = scale[h]
                    value = px * gx_ + py * gy_ + pz * gz_
                    target[h * M + u * 16 : h * M + u * 16 + 16, c * PT : (c + 1) * PT] = value.astype(BF)

    def prepare_cross(v):
        if v == 0:
            weight_copy.wait_recv()
        foreign = swfar[...]
        foreign = jnp.where(odd == 1, pltpu.roll(foreign, LV // 2, 1), foreign)
        wide = [weighted_columns(foreign, v * 32 + 16 * h, 16) for h in range(2)]
        pk = []
        for h in range(2):
            mine = 2 * v + h + 4 * odd
            for c in range(3):
                here = far[2 * v + h, c]
                if c == 0:
                    pk.append(jnp.dot(self_[...], here.T, preferred_element_type=F32).astype(BF))
                at = c * PT + h * CH
                cross_tested[v, :, at : at + CH] = (here.astype(F32) * wide[h]).astype(BF).T
                grads[v][c, :, h * CH : (h + 1) * CH] = planes[c, 0, rows_of(mine), :].T.astype(F32)
            for j in range(JW):
                picks[v][j, :, h * CH : (h + 1) * CH] = jnp.broadcast_to(
                    pk[h][j : j + 1].astype(F32), (8, CH)
                )

    def cross_terms(v, step, target):
        scale = []
        for h in range(2):
            p = picks[v][2 * step + h].astype(BF)
            scale.append(jnp.concatenate([p, p], axis=0))
        for c in range(3):
            for u in range(8):
                tile = grads[v][c, u * 16 : u * 16 + 16, :].astype(BF)
                for h in range(2):
                    target[h * M + u * 16 : h * M + u * 16 + 16, c * PT : (c + 1) * PT] = scale[h] * tile

    stages = [
        (functools.partial(prepare, t), functools.partial(terms, t % 2), lambda t=t: turned[block_of(t)])
        for t in range(8)
    ]
    stages += [
        (functools.partial(prepare_cross, v), functools.partial(cross_terms, v), lambda v=v: cross_tested[v])
        for v in range(2)
    ]
    waiting = None
    stages[0][0]()
    for i, (_, form, tested) in enumerate(stages):
        for step in range(8):
            if waiting is not None:
                waiting()

            def waiting(step=step, tested=tested, fresh=i == 0):
                value = lax.dot_general(
                    tested(),
                    spread[step % 4][...],
                    (((1,), (1,)), ((), ())),
                    preferred_element_type=F32,
                )
                cols = slice(step * 256, step * 256 + 256)
                total[:, cols] = value if fresh else total[:, cols] + value

            form(step, spread[step % 4])
            if step == 3 and i + 1 < len(stages):
                stages[i + 1][0]()
    waiting()

    finish = reduce_parts(total, out, *reduction)
    for k in range(8):
        near_copy(k).wait_send()
        z_copy(0, k).wait_send()
        z_copy(1, k).wait_send()
        if k < 4:
            far_copy(k).wait_send()
    weight_copy.wait_send()
    finish()


VM = pl.BlockSpec(memory_space=pltpu.VMEM)
SM = pl.BlockSpec(memory_space=pltpu.SMEM)
HB = pl.BlockSpec(memory_space=pl.ANY)


def local(modes, weights, counts, mode_index):
    return pl.pallas_call(
        local_kernel,
        out_shape=jax.ShapeDtypeStruct((JW, 4, M), F32),
        in_specs=[HB, HB, SM, SM],
        out_specs=VM,
        scratch_shapes=[
            pltpu.VMEM((2, CZ, LV), F32),
            pltpu.VMEM((M, JW * M), F32),
            pltpu.VMEM((3, 2, ROWS + 2 * PAD, M), BF),
            pltpu.VMEM((8, 3, CH, M), BF),
            pltpu.VMEM((4, 3, CH, M), BF),
            pltpu.VMEM((2, 8, 96, M), BF),
            pltpu.VMEM((2, 8, 96, M), BF),
            pltpu.VMEM((2, CZ, LV), F32),
            pltpu.VMEM((CZ, LV), F32),
            pltpu.VMEM((8, M, 3 * PT), BF),
            pltpu.VMEM((2, M, 3 * PT), BF),
            [pltpu.VMEM((9, M, PT), F32)] * 2,
            [pltpu.VMEM((3 * JW, 8, PT), F32)] * 2,
            [pltpu.VMEM((2 * M, 3 * PT), BF)] * 4,
            pltpu.VMEM((PT, PT), BF),
            pltpu.VMEM((3 * JW, 3 * M), BF),
            pltpu.VMEM((JW, M), BF),
            pltpu.SemaphoreType.DMA((7,)),
            pltpu.SemaphoreType.DMA((8,)),
            pltpu.SemaphoreType.DMA((8,)),
            pltpu.SemaphoreType.DMA((4,)),
            pltpu.SemaphoreType.DMA((4,)),
            pltpu.SemaphoreType.DMA((2, 8)),
            pltpu.SemaphoreType.DMA((2, 8)),
            pltpu.SemaphoreType.DMA((2,)),
            pltpu.VMEM((16, 8, JW * M), F32),
            pltpu.VMEM((16, 8, 8 * M), F32),
            pltpu.VMEM((16, 8, 8 * M), BF),
            pltpu.VMEM((16, 8, 8 * M), BF),
            pltpu.VMEM((2, 4, 8 * M), F32),
            pltpu.VMEM((8, 4, 8 * M), F32),
            pltpu.VMEM((JW, 4, M), F32),
            pltpu.SemaphoreType.DMA((4,)),
            pltpu.SemaphoreType.DMA((4,)),
            pltpu.SemaphoreType.DMA((16,)),
            pltpu.SemaphoreType.DMA((16,)),
            pltpu.SemaphoreType.DMA((8,)),
            pltpu.SemaphoreType.DMA((8,)),
            pltpu.SemaphoreType.DMA((2,)),
        ],
        compiler_params=pltpu.CompilerParams(
            vmem_limit_bytes=67043328, collective_id=0, has_side_effects=True
        ),
    )(modes.reshape(3, 2, ROWS, M), jnp.swapaxes(weights, 1, 2), counts, mode_index)


def solution(mesh):
    placed = (P(None, "gx", None, "gz", None), P("gx", None, "gz"), P(("gx", "gz")), P())
    return jax.shard_map(
        local, mesh=mesh, in_specs=placed, out_specs=P(None, "gz", None), check_vma=False
    )
```

```python
import functools

import jax
import jax.numpy as jnp
from jax import lax
from jax.experimental import pallas as pl
from jax.experimental.pallas import tpu as pltpu
from jax.sharding import PartitionSpec as P

MESH = pl.DeviceIdType.MESH
BF = jnp.bfloat16
F32 = jnp.float32
M = 128
JW = 16
LV = 128
CZ = 8
ROWS = LV * CZ
PAD = 16
CH = 128
PT = 2 * CH
HALF = ROWS // 2


def iota(shape, dim):
    return lax.broadcasted_iota(jnp.int32, shape, dim)


def pick_rows(idx_ref, scales):
    count = len(scales) * JW
    row, col = iota((count, M), 0), iota((count, M), 1)
    wanted = jnp.zeros((count, M), jnp.int32)
    for j in range(JW):
        wanted = jnp.where(row % JW == j, idx_ref[j], wanted)
    blocks = [
        jnp.where((col == wanted) & (row // JW == d), scale, 0.0).astype(BF)
        for d, scale in enumerate(scales)
    ]
    return jnp.concatenate(blocks, axis=1)


def weighted_columns(sw, first, levels):
    return jnp.concatenate(
        [jnp.broadcast_to(sw[:, y : y + 1], (CZ, M)) for y in range(first, first + levels)], axis=0
    )


def stencil_matrix():
    row, col = iota((PT, PT), 0), iota((PT, PT), 1)
    point = lax.rem(col, CH)
    lev, z = point // CZ, lax.rem(point, CZ)
    up = jnp.where(point + CZ < CH, point + CZ, point + CZ + 16)
    down = jnp.where(point >= CZ, point - CZ, CH + 8 + point)
    ahead = jnp.where(z < CZ - 1, point + 1, CH + 48 + lev)
    behind = jnp.where(z > 0, point - 1, CH + 32 + lev)
    plus = jnp.where(col < CH, up, ahead)
    minus = jnp.where(col < CH, down, behind)
    return (jnp.where(row == plus, 1.0, 0.0) - jnp.where(row == minus, 1.0, 0.0)).astype(BF)


def select_rows():
    row, col = iota((32, CH), 0), iota((32, CH), 1)
    return jnp.where(col == lax.rem(row, 16) * CZ + (row // 16) * (CZ - 1), 1.0, 0.0).astype(BF)


def place():
    gx, gz = lax.axis_index("gx"), lax.axis_index("gz")
    core, zh = lax.rem(gx, 2), gx // 2
    x, low, y = gz // 8, lax.rem(gz // 4, 2), lax.rem(gz, 4)
    return gx, gz, core, x, low, y, x * 4 + y, zh * 2 + low


def plane_peer(p):
    gx, _, _, _, low, _, _, _ = place()
    return (gx, (p // 4) * 8 + low * 4 + lax.rem(p, 4))


def column_peer(p):
    _, _, core, x, _, y, _, _ = place()
    return ((p // 2) * 2 + core, x * 8 + lax.rem(p, 2) * 4 + y)


def reduction_peers():
    _, _, _, _, _, _, q, z = place()
    return [plane_peer(lax.rem(q + d, 16)) for d in range(1, 16)] + [
        column_peer(lax.rem(z + d, 8)) for d in range(1, 8)
    ]


def reduce_parts(
    total, out, part, pair, send, got, column, stack, whole, asend, arecv, bsend, brecv, csend, crecv, dsem
):
    gx, gz, core, x, low, y, q, z = place()
    partner = (gx + 1 - 2 * core, gz)

    width = 8 * M
    own = pl.ds(pl.multiple_of(core * width, width), width)
    theirs = pl.ds(pl.multiple_of((1 - core) * width, width), width)

    def pair_copy(g):
        quarter = pl.ds(g * 4, 4)
        return pltpu.make_async_remote_copy(
            src_ref=part.at[quarter, :, theirs],
            dst_ref=pair.at[quarter],
            send_sem=asend.at[g],
            recv_sem=arecv.at[g],
            device_id=partner,
            device_id_type=MESH,
        )

    def plane_copy(dest, slot):
        return pltpu.make_async_remote_copy(
            src_ref=send.at[dest],
            dst_ref=got.at[slot],
            send_sem=bsend.at[dest],
            recv_sem=brecv.at[slot],
            device_id=plane_peer(dest),
            device_id_type=MESH,
        )

    def column_copy(dest, slot):
        return pltpu.make_async_remote_copy(
            src_ref=column.at[lax.rem(dest, 2)],
            dst_ref=stack.at[slot],
            send_sem=csend.at[dest],
            recv_sem=crecv.at[slot],
            device_id=column_peer(dest),
            device_id_type=MESH,
        )

    for g in range(4):
        for b in range(g * 4, g * 4 + 4):
            for half in range(2):
                owner = (b // 4) * 8 + half * 4 + b % 4
                part[b, half * 4 : half * 4 + 4, :] = total[owner * 4 : owner * 4 + 4, :]
        pair_copy(g).start()
    for g in range(4):
        pair_copy(g).wait_recv()
        for b in range(g * 4, g * 4 + 4):
            send[b] = (part[b, :, own] + pair[b]).astype(BF)

            @pl.when(b != q)
            def _(b=b):
                plane_copy(b, q).start()

    mine = send[q].astype(F32)
    for d in range(1, 16):
        p = lax.rem(q + d, 16)
        plane_copy(p, p).wait_recv()
        mine = mine + got[p].astype(F32)
    column[0] = mine[:4].astype(BF)
    column[1] = mine[4:].astype(BF)
    for d in (4, 3, 5, 2, 6, 1, 7):
        column_copy(lax.rem(z + d, 8), z).start()
    stack[z] = column[low]
    for d in range(1, 8):
        p = lax.rem(z + d, 8)
        column_copy(p, p).wait_recv()
    mine = stack[0].astype(F32)
    for p in range(1, 8):
        mine = mine + stack[p].astype(F32)
    for j in range(8):
        whole[core * 8 + j] = mine[:, j * M : (j + 1) * M]
    block = whole.at[pl.ds(core * 8, 8)]
    last = pltpu.make_async_remote_copy(
        src_ref=block, dst_ref=block, send_sem=dsem.at[0], recv_sem=dsem.at[1],
        device_id=partner, device_id_type=MESH,
    )
    last.start()
    last.wait_recv()
    out[...] = whole[...]

    def finish():
        for g in range(4):
            pair_copy(g).wait_send()
        for d in range(1, 16):
            plane_copy(lax.rem(q + d, 16), q).wait_send()
        for d in range(1, 8):
            column_copy(lax.rem(z + d, 8), z).wait_send()
        last.wait_send()

    return finish


def local_kernel(
    modes, weights, counts, idx, out,
    weights_in, total, planes, near, far, zsend, zgot, sw, swfar, turned, cross_tested, grads, picks, spread, stencil, sel, self_,
    local_sem, near_s, near_r, far_s, far_r, z_s, z_r, w_sem, *reduction,
):
    gx, gz = lax.axis_index("gx"), lax.axis_index("gz")
    odd = lax.rem(gx, 2)
    sign = jnp.where(odd == 0, 0.5, -0.5).astype(F32)
    near_peer = (gx + 1 - 2 * odd, gz)
    far_peer = (lax.rem(gx + 7 + 2 * odd, 8), gz)
    z_peers = ((gx, lax.rem(gz + 31, 32)), (gx, lax.rem(gz + 1, 32)))

    barrier = pltpu.get_barrier_semaphore()
    peers = [near_peer, far_peer, *z_peers, *reduction_peers()]
    for peer in peers:
        pl.semaphore_signal(barrier, inc=1, device_id=peer, device_id_type=MESH)
    small = [pltpu.make_async_copy(weights, weights_in, local_sem.at[6])]
    copies = []
    for c in range(3):
        for side in range(2):
            which = odd if side == 0 else 1 - odd
            copies.append(
                pltpu.make_async_copy(
                    modes.at[c, which], planes.at[c, side, pl.ds(PAD, ROWS)], local_sem.at[2 * c + side]
                )
            )
    for copy in (*small, *copies):
        copy.start()
    for c in range(3):
        for side in range(2):
            planes[c, side, pl.ds(0, PAD), :] = jnp.zeros((PAD, M), BF)
            planes[c, side, pl.ds(PAD + ROWS, PAD), :] = jnp.zeros((PAD, M), BF)
    for copy in small:
        copy.wait()
    for side in range(2):
        which = odd if side == 0 else 1 - odd
        w = weights_in[which]
        sw[side] = jnp.where(iota((CZ, LV), 1) < counts[0], w, jnp.zeros_like(w))
    stencil[...] = stencil_matrix()
    sel[...] = pick_rows(idx, (sign, 0.5, 0.5))
    self_[...] = pick_rows(idx, (sign,))
    ends = select_rows()
    for copy in copies:
        copy.wait()

    def block_of(t):
        return lax.rem(t + 4 * (1 - odd), 8)

    def rows_of(k):
        return pl.ds(pl.multiple_of(PAD + k * CH, 16), CH)

    def near_copy(k):
        return pltpu.make_async_remote_copy(
            src_ref=planes.at[:, 1, rows_of(k)], dst_ref=near.at[k],
            send_sem=near_s.at[k], recv_sem=near_r.at[k], device_id=near_peer, device_id_type=MESH,
        )

    def far_copy(p):
        return pltpu.make_async_remote_copy(
            src_ref=planes.at[:, 0, rows_of(p + 4 * (1 - odd))], dst_ref=far.at[p],
            send_sem=far_s.at[p], recv_sem=far_r.at[p], device_id=far_peer, device_id_type=MESH,
        )

    def z_copy(direction, k):
        return pltpu.make_async_remote_copy(
            src_ref=zsend.at[direction, k], dst_ref=zgot.at[direction, k],
            send_sem=z_s.at[direction, k], recv_sem=z_r.at[direction, k],
            device_id=z_peers[direction], device_id_type=MESH,
        )

    weight_copy = pltpu.make_async_remote_copy(
        src_ref=sw.at[0], dst_ref=swfar, send_sem=w_sem.at[0], recv_sem=w_sem.at[1],
        device_id=far_peer, device_id_type=MESH,
    )

    def send_edges(t, carry):
        k = block_of(t)
        for c in range(3):
            for side in range(2):
                edge = jnp.dot(ends, planes[c, side, rows_of(k), :], preferred_element_type=F32).astype(BF)
                at = (2 * c + side) * 16
                zsend[0, k, at : at + 16, :] = edge[:16]
                zsend[1, k, at : at + 16, :] = edge[16:]
        return carry

    lax.fori_loop(0, 8, send_edges, 0)
    pl.semaphore_wait(barrier, len(peers))
    for t in range(8):
        near_copy(lax.rem(t + 4 * odd, 8)).start()
        z_copy(0, block_of(t)).start()
        z_copy(1, block_of(t)).start()
    for p in range(4):
        far_copy(p).start()
    weight_copy.start()
    for k in range(8):
        for side in range(2):
            wide = weighted_columns(sw[side], k * 16, 16)
            for c in range(3):
                here = planes[c, side, PAD + k * CH : PAD + (k + 1) * CH, :].astype(F32)
                at = c * PT + side * CH
                turned[k, :, at : at + CH] = (here * wide).astype(BF).T

    def prepare(t, b):
        k, with_far = block_of(t), t >= 4
        near_copy(k).wait_recv()
        z_copy(0, k).wait_recv()
        z_copy(1, k).wait_recv()
        if with_far:
            far_copy(t - 4).wait_recv()
        g = grads[b]
        flipped = [[], []]
        for side in range(2):
            lanes = slice(side * CH, (side + 1) * CH)
            for c in range(3):
                at = (2 * c + side) * 16
                stacked = jnp.concatenate(
                    [
                        planes[c, side, rows_of(k), :],
                        planes[c, side, pl.ds(pl.multiple_of(k * CH, 16), 16), :],
                        planes[c, side, pl.ds(pl.multiple_of(PAD + (k + 1) * CH, 16), 16), :],
                        zgot[1, k, at : at + 16, :],
                        zgot[0, k, at : at + 16, :],
                        jnp.zeros((64, M), BF),
                    ],
                    axis=0,
                ).T
                both = jnp.dot(stacked, stencil[...], preferred_element_type=F32)
                g[3 + c, :, lanes] = both[:, :CH]
                g[6 + c, :, lanes] = both[:, CH:]
                flipped[side].append(stacked[:, :CH])
            pk = jnp.dot(sel[...], jnp.concatenate(flipped[side], axis=0), preferred_element_type=F32)
            for r in range(3 * JW):
                picks[b][r, :, lanes] = jnp.broadcast_to(pk[r : r + 1], (8, CH))
        for c in range(3):
            inner = flipped[1][c].astype(F32)
            if with_far:
                inner = inner - far[t - 4, c].T.astype(F32)
            g[c, :, :CH] = inner
            g[c, :, CH:] = near[k, c].T.astype(F32) - flipped[0][c].astype(F32)

    def terms(b, step, target):
        g, pk = grads[b], picks[b]
        scale = []
        for h in range(2):
            p = [pk[d * JW + 2 * step + h] for d in range(3)]
            scale.append([jnp.concatenate([v, v], axis=0) for v in p])
        for c in range(3):
            for u in range(8):
                tile = slice(u * 16, u * 16 + 16)
                gx_, gy_, gz_ = g[c, tile, :], g[3 + c, tile, :], g[6 + c, tile, :]
                for h in range(2):
                    px, py, pz = scale[h]
                    value = px * gx_ + py * gy_ + pz * gz_
                    target[h * M + u * 16 : h * M + u * 16 + 16, c * PT : (c + 1) * PT] = value.astype(BF)

    def prepare_cross(v, b):
        if v == 0:
            weight_copy.wait_recv()
        foreign = swfar[...]
        foreign = jnp.where(odd == 1, pltpu.roll(foreign, LV // 2, 1), foreign)
        wide = [weighted_columns(foreign, v * 32 + 16 * h, 16) for h in range(2)]
        pk = []
        for h in range(2):
            mine = 2 * v + h + 4 * odd
            for c in range(3):
                here = far[2 * v + h, c]
                if c == 0:
                    pk.append(jnp.dot(self_[...], here.T, preferred_element_type=F32).astype(BF))
                at = c * PT + h * CH
                cross_tested[v, :, at : at + CH] = (here.astype(F32) * wide[h]).astype(BF).T
                grads[b][c, :, h * CH : (h + 1) * CH] = planes[c, 0, rows_of(mine), :].T.astype(F32)
            for j in range(JW):
                picks[b][j, :, h * CH : (h + 1) * CH] = jnp.broadcast_to(
                    pk[h][j : j + 1].astype(F32), (8, CH)
                )

    def cross_terms(b, step, target):
        scale = []
        for h in range(2):
            p = picks[b][2 * step + h].astype(BF)
            scale.append(jnp.concatenate([p, p], axis=0))
        for c in range(3):
            for u in range(8):
                tile = grads[b][c, u * 16 : u * 16 + 16, :].astype(BF)
                for h in range(2):
                    target[h * M + u * 16 : h * M + u * 16 + 16, c * PT : (c + 1) * PT] = scale[h] * tile

    stages = []
    for kind, n in [(0, t) for t in range(6)] + [(1, 0), (0, 6), (0, 7), (1, 1)]:
        b = len(stages) % 2
        if kind == 0:
            made, form = functools.partial(prepare, n, b), functools.partial(terms, b)
            stages.append((made, form, lambda n=n: turned[block_of(n)]))
        else:
            made, form = functools.partial(prepare_cross, n, b), functools.partial(cross_terms, b)
            stages.append((made, form, lambda n=n: cross_tested[n]))
    waiting = None
    stages[0][0]()
    for i, (_, form, tested) in enumerate(stages):
        for step in range(8):
            if waiting is not None:
                waiting()

            def waiting(step=step, tested=tested, fresh=i == 0):
                value = lax.dot_general(
                    tested(),
                    spread[step % 4][...],
                    (((1,), (1,)), ((), ())),
                    preferred_element_type=F32,
                )
                cols = slice(step * 256, step * 256 + 256)
                total[:, cols] = value if fresh else total[:, cols] + value

            form(step, spread[step % 4])
            if step == 3 and i + 1 < len(stages):
                stages[i + 1][0]()
    waiting()

    finish = reduce_parts(total, out, *reduction)
    for k in range(8):
        near_copy(k).wait_send()
        z_copy(0, k).wait_send()
        z_copy(1, k).wait_send()
        if k < 4:
            far_copy(k).wait_send()
    weight_copy.wait_send()
    finish()


VM = pl.BlockSpec(memory_space=pltpu.VMEM)
SM = pl.BlockSpec(memory_space=pltpu.SMEM)
HB = pl.BlockSpec(memory_space=pl.ANY)


def local(modes, weights, counts, mode_index):
    return pl.pallas_call(
        local_kernel,
        out_shape=jax.ShapeDtypeStruct((JW, 4, M), F32),
        in_specs=[HB, HB, SM, SM],
        out_specs=VM,
        scratch_shapes=[
            pltpu.VMEM((2, CZ, LV), F32),
            pltpu.VMEM((M, JW * M), F32),
            pltpu.VMEM((3, 2, ROWS + 2 * PAD, M), BF),
            pltpu.VMEM((8, 3, CH, M), BF),
            pltpu.VMEM((4, 3, CH, M), BF),
            pltpu.VMEM((2, 8, 96, M), BF),
            pltpu.VMEM((2, 8, 96, M), BF),
            pltpu.VMEM((2, CZ, LV), F32),
            pltpu.VMEM((CZ, LV), F32),
            pltpu.VMEM((8, M, 3 * PT), BF),
            pltpu.VMEM((2, M, 3 * PT), BF),
            [pltpu.VMEM((9, M, PT), F32)] * 2,
            [pltpu.VMEM((3 * JW, 8, PT), F32)] * 2,
            [pltpu.VMEM((2 * M, 3 * PT), BF)] * 4,
            pltpu.VMEM((PT, PT), BF),
            pltpu.VMEM((3 * JW, 3 * M), BF),
            pltpu.VMEM((JW, M), BF),
            pltpu.SemaphoreType.DMA((7,)),
            pltpu.SemaphoreType.DMA((8,)),
            pltpu.SemaphoreType.DMA((8,)),
            pltpu.SemaphoreType.DMA((4,)),
            pltpu.SemaphoreType.DMA((4,)),
            pltpu.SemaphoreType.DMA((2, 8)),
            pltpu.SemaphoreType.DMA((2, 8)),
            pltpu.SemaphoreType.DMA((2,)),
            pltpu.VMEM((16, 8, JW * M), F32),
            pltpu.VMEM((16, 8, 8 * M), F32),
            pltpu.VMEM((16, 8, 8 * M), BF),
            pltpu.VMEM((16, 8, 8 * M), BF),
            pltpu.VMEM((2, 4, 8 * M), BF),
            pltpu.VMEM((8, 4, 8 * M), BF),
            pltpu.VMEM((JW, 4, M), F32),
            pltpu.SemaphoreType.DMA((4,)),
            pltpu.SemaphoreType.DMA((4,)),
            pltpu.SemaphoreType.DMA((16,)),
            pltpu.SemaphoreType.DMA((16,)),
            pltpu.SemaphoreType.DMA((8,)),
            pltpu.SemaphoreType.DMA((8,)),
            pltpu.SemaphoreType.DMA((2,)),
        ],
        compiler_params=pltpu.CompilerParams(
            vmem_limit_bytes=67043328, collective_id=0, has_side_effects=True
        ),
    )(modes.reshape(3, 2, ROWS, M), jnp.swapaxes(weights, 1, 2), counts, mode_index)


def solution(mesh):
    placed = (P(None, "gx", None, "gz", None), P("gx", None, "gz"), P(("gx", "gz")), P())
    return jax.shard_map(
        local, mesh=mesh, in_specs=placed, out_specs=P(None, "gz", None), check_vma=False
    )
```

```python
import functools

import jax
import jax.numpy as jnp
from jax import lax
from jax.experimental import pallas as pl
from jax.experimental.pallas import tpu as pltpu
from jax.sharding import PartitionSpec as P

MESH = pl.DeviceIdType.MESH
BF = jnp.bfloat16
F32 = jnp.float32
M = 128
JW = 16
LV = 128
CZ = 8
ROWS = LV * CZ
PAD = 16
CH = 128
PT = 2 * CH
HALF = ROWS // 2


def iota(shape, dim):
    return lax.broadcasted_iota(jnp.int32, shape, dim)


def pick_rows(idx_ref, scales):
    count = len(scales) * JW
    row, col = iota((count, M), 0), iota((count, M), 1)
    wanted = jnp.zeros((count, M), jnp.int32)
    for j in range(JW):
        wanted = jnp.where(row % JW == j, idx_ref[j], wanted)
    blocks = [
        jnp.where((col == wanted) & (row // JW == d), scale, 0.0).astype(BF)
        for d, scale in enumerate(scales)
    ]
    return jnp.concatenate(blocks, axis=1)


def weighted_columns(sw, first, levels):
    return jnp.concatenate(
        [jnp.broadcast_to(sw[:, y : y + 1], (CZ, M)) for y in range(first, first + levels)], axis=0
    )


def stencil_matrix():
    row, col = iota((PT, PT), 0), iota((PT, PT), 1)
    point = lax.rem(col, CH)
    lev, z = point // CZ, lax.rem(point, CZ)
    up = jnp.where(point + CZ < CH, point + CZ, point + CZ + 16)
    down = jnp.where(point >= CZ, point - CZ, CH + 8 + point)
    ahead = jnp.where(z < CZ - 1, point + 1, CH + 48 + lev)
    behind = jnp.where(z > 0, point - 1, CH + 32 + lev)
    plus = jnp.where(col < CH, up, ahead)
    minus = jnp.where(col < CH, down, behind)
    return (jnp.where(row == plus, 1.0, 0.0) - jnp.where(row == minus, 1.0, 0.0)).astype(BF)


def select_rows():
    row, col = iota((32, CH), 0), iota((32, CH), 1)
    return jnp.where(col == lax.rem(row, 16) * CZ + (row // 16) * (CZ - 1), 1.0, 0.0).astype(BF)


def place():
    gx, gz = lax.axis_index("gx"), lax.axis_index("gz")
    core, zh = lax.rem(gx, 2), gx // 2
    x, low, y = gz // 8, lax.rem(gz // 4, 2), lax.rem(gz, 4)
    return gx, gz, core, x, low, y, x * 4 + y, zh * 2 + low


def plane_peer(p):
    gx, _, _, _, low, _, _, _ = place()
    return (gx, (p // 4) * 8 + low * 4 + lax.rem(p, 4))


def column_peer(p):
    _, _, core, x, _, y, _, _ = place()
    return ((p // 2) * 2 + core, x * 8 + lax.rem(p, 2) * 4 + y)


def reduction_peers():
    _, _, _, _, _, _, q, z = place()
    return [plane_peer(lax.rem(q + d, 16)) for d in range(1, 16)] + [
        column_peer(lax.rem(z + d, 8)) for d in range(1, 8)
    ]


def reduce_parts(
    total, out, part, pair, send, got, column, stack, whole, asend, arecv, bsend, brecv, csend, crecv, dsem
):
    gx, gz, core, x, low, y, q, z = place()
    partner = (gx + 1 - 2 * core, gz)

    width = 8 * M
    own = pl.ds(pl.multiple_of(core * width, width), width)
    theirs = pl.ds(pl.multiple_of((1 - core) * width, width), width)

    def pair_copy(g):
        quarter = pl.ds(g * 4, 4)
        return pltpu.make_async_remote_copy(
            src_ref=part.at[quarter, :, theirs],
            dst_ref=pair.at[quarter],
            send_sem=asend.at[g],
            recv_sem=arecv.at[g],
            device_id=partner,
            device_id_type=MESH,
        )

    def plane_copy(dest, slot):
        return pltpu.make_async_remote_copy(
            src_ref=send.at[dest],
            dst_ref=got.at[slot],
            send_sem=bsend.at[dest],
            recv_sem=brecv.at[slot],
            device_id=plane_peer(dest),
            device_id_type=MESH,
        )

    def column_copy(dest, slot):
        return pltpu.make_async_remote_copy(
            src_ref=column.at[lax.rem(dest, 2)],
            dst_ref=stack.at[slot],
            send_sem=csend.at[dest],
            recv_sem=crecv.at[slot],
            device_id=column_peer(dest),
            device_id_type=MESH,
        )

    for g in range(4):
        for b in range(g * 4, g * 4 + 4):
            for half in range(2):
                owner = (b // 4) * 8 + half * 4 + b % 4
                part[b, half * 4 : half * 4 + 4, :] = total[owner * 4 : owner * 4 + 4, :]
        pair_copy(g).start()
    for g in range(4):
        pair_copy(g).wait_recv()
        for b in range(g * 4, g * 4 + 4):
            send[b] = (part[b, :, own] + pair[b]).astype(BF)

            @pl.when(b != q)
            def _(b=b):
                plane_copy(b, q).start()

    mine = send[q].astype(F32)
    for d in range(1, 16):
        p = lax.rem(q + d, 16)
        plane_copy(p, p).wait_recv()
        mine = mine + got[p].astype(F32)
    column[0] = mine[:4].astype(BF)
    column[1] = mine[4:].astype(BF)
    for d in (4, 3, 5, 2, 6, 1, 7):
        column_copy(lax.rem(z + d, 8), z).start()
    stack[z] = column[low]
    for d in range(1, 8):
        p = lax.rem(z + d, 8)
        column_copy(p, p).wait_recv()
    mine = stack[0].astype(F32)
    for p in range(1, 8):
        mine = mine + stack[p].astype(F32)
    for j in range(8):
        whole[core * 8 + j] = mine[:, j * M : (j + 1) * M]
    block = whole.at[pl.ds(core * 8, 8)]
    last = pltpu.make_async_remote_copy(
        src_ref=block, dst_ref=block, send_sem=dsem.at[0], recv_sem=dsem.at[1],
        device_id=partner, device_id_type=MESH,
    )
    last.start()
    last.wait_recv()
    out[...] = whole[...]

    def finish():
        for g in range(4):
            pair_copy(g).wait_send()
        for d in range(1, 16):
            plane_copy(lax.rem(q + d, 16), q).wait_send()
        for d in range(1, 8):
            column_copy(lax.rem(z + d, 8), z).wait_send()
        last.wait_send()

    return finish


def local_kernel(
    modes, weights, counts, idx, out,
    weights_in, total, planes, near, far, zsend, zgot, sw, swfar, turned, cross_tested, grads, picks, spread, stencil, sel, self_,
    local_sem, near_s, near_r, far_s, far_r, z_s, z_r, w_sem, *reduction,
):
    gx, gz = lax.axis_index("gx"), lax.axis_index("gz")
    odd = lax.rem(gx, 2)
    sign = jnp.where(odd == 0, 0.5, -0.5).astype(F32)
    near_peer = (gx + 1 - 2 * odd, gz)
    far_peer = (lax.rem(gx + 7 + 2 * odd, 8), gz)
    z_peers = ((gx, lax.rem(gz + 31, 32)), (gx, lax.rem(gz + 1, 32)))

    barrier = pltpu.get_barrier_semaphore()
    peers = [near_peer, far_peer, *z_peers, *reduction_peers()]
    for peer in peers:
        pl.semaphore_signal(barrier, inc=1, device_id=peer, device_id_type=MESH)
    small = [pltpu.make_async_copy(weights, weights_in, local_sem.at[6])]
    copies = []
    for c in range(3):
        for side in range(2):
            which = odd if side == 0 else 1 - odd
            copies.append(
                pltpu.make_async_copy(
                    modes.at[c, which], planes.at[c, side, pl.ds(PAD, ROWS)], local_sem.at[2 * c + side]
                )
            )
    for copy in (*small, *copies):
        copy.start()
    for c in range(3):
        for side in range(2):
            planes[c, side, pl.ds(0, PAD), :] = jnp.zeros((PAD, M), BF)
            planes[c, side, pl.ds(PAD + ROWS, PAD), :] = jnp.zeros((PAD, M), BF)
    for copy in small:
        copy.wait()
    for side in range(2):
        which = odd if side == 0 else 1 - odd
        w = weights_in[which]
        sw[side] = jnp.where(iota((CZ, LV), 1) < counts[0], w, jnp.zeros_like(w))
    stencil[...] = stencil_matrix()
    sel[...] = pick_rows(idx, (sign, 0.5, 0.5))
    self_[...] = pick_rows(idx, (sign,))
    ends = select_rows()
    for copy in copies:
        copy.wait()

    def block_of(t):
        return lax.rem(t + 4 * (1 - odd), 8)

    def rows_of(k):
        return pl.ds(pl.multiple_of(PAD + k * CH, 16), CH)

    def near_copy(k):
        return pltpu.make_async_remote_copy(
            src_ref=planes.at[:, 1, rows_of(k)], dst_ref=near.at[k],
            send_sem=near_s.at[k], recv_sem=near_r.at[k], device_id=near_peer, device_id_type=MESH,
        )

    def far_copy(p):
        return pltpu.make_async_remote_copy(
            src_ref=planes.at[:, 0, rows_of(p + 4 * (1 - odd))], dst_ref=far.at[p],
            send_sem=far_s.at[p], recv_sem=far_r.at[p], device_id=far_peer, device_id_type=MESH,
        )

    def z_copy(direction, k):
        return pltpu.make_async_remote_copy(
            src_ref=zsend.at[direction, k], dst_ref=zgot.at[direction, k],
            send_sem=z_s.at[direction, k], recv_sem=z_r.at[direction, k],
            device_id=z_peers[direction], device_id_type=MESH,
        )

    weight_copy = pltpu.make_async_remote_copy(
        src_ref=sw.at[0], dst_ref=swfar, send_sem=w_sem.at[0], recv_sem=w_sem.at[1],
        device_id=far_peer, device_id_type=MESH,
    )

    def send_edges(t, carry):
        k = block_of(t)
        for c in range(3):
            for side in range(2):
                edge = jnp.dot(ends, planes[c, side, rows_of(k), :], preferred_element_type=F32).astype(BF)
                at = (2 * c + side) * 16
                zsend[0, k, at : at + 16, :] = edge[:16]
                zsend[1, k, at : at + 16, :] = edge[16:]
        return carry

    lax.fori_loop(0, 8, send_edges, 0)
    pl.semaphore_wait(barrier, len(peers))
    for t in range(8):
        near_copy(lax.rem(t + 4 * odd, 8)).start()
        z_copy(0, block_of(t)).start()
        z_copy(1, block_of(t)).start()
    for p in range(4):
        far_copy(p).start()
    weight_copy.start()
    for k in range(8):
        for side in range(2):
            wide = weighted_columns(sw[side], k * 16, 16)
            for c in range(3):
                here = planes[c, side, PAD + k * CH : PAD + (k + 1) * CH, :].astype(F32)
                at = c * PT + side * CH
                turned[k, :, at : at + CH] = (here * wide).astype(BF).T

    def prepare(t, b):
        k, with_far = block_of(t), t >= 4
        near_copy(k).wait_recv()
        z_copy(0, k).wait_recv()
        z_copy(1, k).wait_recv()
        if with_far:
            far_copy(t - 4).wait_recv()
        g = grads[b]
        flipped = [[], []]
        for side in range(2):
            lanes = slice(side * CH, (side + 1) * CH)
            for c in range(3):
                at = (2 * c + side) * 16
                stacked = jnp.concatenate(
                    [
                        planes[c, side, rows_of(k), :],
                        planes[c, side, pl.ds(pl.multiple_of(k * CH, 16), 16), :],
                        planes[c, side, pl.ds(pl.multiple_of(PAD + (k + 1) * CH, 16), 16), :],
                        zgot[1, k, at : at + 16, :],
                        zgot[0, k, at : at + 16, :],
                        jnp.zeros((64, M), BF),
                    ],
                    axis=0,
                ).T
                both = jnp.dot(stacked, stencil[...], preferred_element_type=F32)
                g[3 + c, :, lanes] = both[:, :CH]
                g[6 + c, :, lanes] = both[:, CH:]
                flipped[side].append(stacked[:, :CH])
            pk = jnp.dot(sel[...], jnp.concatenate(flipped[side], axis=0), preferred_element_type=F32)
            for r in range(3 * JW):
                picks[b][r, :, lanes] = jnp.broadcast_to(pk[r : r + 1], (8, CH))
        for c in range(3):
            inner = flipped[1][c].astype(F32)
            if with_far:
                inner = inner - far[t - 4, c].T.astype(F32)
            g[c, :, :CH] = inner
            g[c, :, CH:] = near[k, c].T.astype(F32) - flipped[0][c].astype(F32)

    def terms(b, step, target):
        g, pk = grads[b], picks[b]
        scale = []
        for h in range(2):
            p = [pk[d * JW + 2 * step + h] for d in range(3)]
            scale.append([jnp.concatenate([v, v], axis=0) for v in p])
        for c in range(3):
            for u in range(8):
                tile = slice(u * 16, u * 16 + 16)
                gx_, gy_, gz_ = g[c, tile, :], g[3 + c, tile, :], g[6 + c, tile, :]
                for h in range(2):
                    px, py, pz = scale[h]
                    value = px * gx_ + py * gy_ + pz * gz_
                    target[h * M + u * 16 : h * M + u * 16 + 16, c * PT : (c + 1) * PT] = value.astype(BF)

    def prepare_cross(v, b):
        if v == 0:
            weight_copy.wait_recv()
        foreign = swfar[...]
        foreign = jnp.where(odd == 1, pltpu.roll(foreign, LV // 2, 1), foreign)
        wide = [weighted_columns(foreign, v * 32 + 16 * h, 16) for h in range(2)]
        pk = []
        for h in range(2):
            mine = 2 * v + h + 4 * odd
            for c in range(3):
                here = far[2 * v + h, c]
                if c == 0:
                    pk.append(jnp.dot(self_[...], here.T, preferred_element_type=F32).astype(BF))
                at = c * PT + h * CH
                cross_tested[v, :, at : at + CH] = (here.astype(F32) * wide[h]).astype(BF).T
                grads[b][c, :, h * CH : (h + 1) * CH] = planes[c, 0, rows_of(mine), :].T.astype(F32)
            for j in range(JW):
                picks[b][j, :, h * CH : (h + 1) * CH] = jnp.broadcast_to(
                    pk[h][j : j + 1].astype(F32), (8, CH)
                )

    def cross_terms(b, step, target):
        scale = []
        for h in range(2):
            p = picks[b][2 * step + h].astype(BF)
            scale.append(jnp.concatenate([p, p], axis=0))
        for c in range(3):
            for u in range(8):
                tile = grads[b][c, u * 16 : u * 16 + 16, :].astype(BF)
                for h in range(2):
                    target[h * M + u * 16 : h * M + u * 16 + 16, c * PT : (c + 1) * PT] = scale[h] * tile

    stages = []
    for kind, n in [(0, t) for t in range(6)] + [(1, 0), (0, 6), (0, 7), (1, 1)]:
        b = len(stages) % 2
        if kind == 0:
            made, form = functools.partial(prepare, n, b), functools.partial(terms, b)
            stages.append((made, form, lambda n=n: turned[block_of(n)]))
        else:
            made, form = functools.partial(prepare_cross, n, b), functools.partial(cross_terms, b)
            stages.append((made, form, lambda n=n: cross_tested[n]))
    waiting = None
    stages[0][0]()
    for i, (_, form, tested) in enumerate(stages):
        for step in range(8):
            if waiting is not None:
                waiting()

            def waiting(step=step, tested=tested, fresh=i == 0):
                value = lax.dot_general(
                    tested(),
                    spread[step % 4][...],
                    (((1,), (1,)), ((), ())),
                    preferred_element_type=F32,
                )
                cols = slice(step * 256, step * 256 + 256)
                total[:, cols] = value if fresh else total[:, cols] + value

            form(step, spread[step % 4])
            if step == 5 and i + 1 < len(stages):
                stages[i + 1][0]()
    waiting()

    finish = reduce_parts(total, out, *reduction)
    for k in range(8):
        near_copy(k).wait_send()
        z_copy(0, k).wait_send()
        z_copy(1, k).wait_send()
        if k < 4:
            far_copy(k).wait_send()
    weight_copy.wait_send()
    finish()


VM = pl.BlockSpec(memory_space=pltpu.VMEM)
SM = pl.BlockSpec(memory_space=pltpu.SMEM)
HB = pl.BlockSpec(memory_space=pl.ANY)


def local(modes, weights, counts, mode_index):
    return pl.pallas_call(
        local_kernel,
        out_shape=jax.ShapeDtypeStruct((JW, 4, M), F32),
        in_specs=[HB, HB, SM, SM],
        out_specs=VM,
        scratch_shapes=[
            pltpu.VMEM((2, CZ, LV), F32),
            pltpu.VMEM((M, JW * M), F32),
            pltpu.VMEM((3, 2, ROWS + 2 * PAD, M), BF),
            pltpu.VMEM((8, 3, CH, M), BF),
            pltpu.VMEM((4, 3, CH, M), BF),
            pltpu.VMEM((2, 8, 96, M), BF),
            pltpu.VMEM((2, 8, 96, M), BF),
            pltpu.VMEM((2, CZ, LV), F32),
            pltpu.VMEM((CZ, LV), F32),
            pltpu.VMEM((8, M, 3 * PT), BF),
            pltpu.VMEM((2, M, 3 * PT), BF),
            [pltpu.VMEM((9, M, PT), F32)] * 2,
            [pltpu.VMEM((3 * JW, 8, PT), F32)] * 2,
            [pltpu.VMEM((2 * M, 3 * PT), BF)] * 4,
            pltpu.VMEM((PT, PT), BF),
            pltpu.VMEM((3 * JW, 3 * M), BF),
            pltpu.VMEM((JW, M), BF),
            pltpu.SemaphoreType.DMA((7,)),
            pltpu.SemaphoreType.DMA((8,)),
            pltpu.SemaphoreType.DMA((8,)),
            pltpu.SemaphoreType.DMA((4,)),
            pltpu.SemaphoreType.DMA((4,)),
            pltpu.SemaphoreType.DMA((2, 8)),
            pltpu.SemaphoreType.DMA((2, 8)),
            pltpu.SemaphoreType.DMA((2,)),
            pltpu.VMEM((16, 8, JW * M), F32),
            pltpu.VMEM((16, 8, 8 * M), F32),
            pltpu.VMEM((16, 8, 8 * M), BF),
            pltpu.VMEM((16, 8, 8 * M), BF),
            pltpu.VMEM((2, 4, 8 * M), BF),
            pltpu.VMEM((8, 4, 8 * M), BF),
            pltpu.VMEM((JW, 4, M), F32),
            pltpu.SemaphoreType.DMA((4,)),
            pltpu.SemaphoreType.DMA((4,)),
            pltpu.SemaphoreType.DMA((16,)),
            pltpu.SemaphoreType.DMA((16,)),
            pltpu.SemaphoreType.DMA((8,)),
            pltpu.SemaphoreType.DMA((8,)),
            pltpu.SemaphoreType.DMA((2,)),
        ],
        compiler_params=pltpu.CompilerParams(
            vmem_limit_bytes=67043328, collective_id=0, has_side_effects=True
        ),
    )(modes.reshape(3, 2, ROWS, M), jnp.swapaxes(weights, 1, 2), counts, mode_index)


def solution(mesh):
    placed = (P(None, "gx", None, "gz", None), P("gx", None, "gz"), P(("gx", "gz")), P())
    return jax.shard_map(
        local, mesh=mesh, in_specs=placed, out_specs=P(None, "gz", None), check_vma=False
    )
```

```python
import functools

import jax
import jax.numpy as jnp
from jax import lax
from jax.experimental import pallas as pl
from jax.experimental.pallas import tpu as pltpu
from jax.sharding import PartitionSpec as P

MESH = pl.DeviceIdType.MESH
BF = jnp.bfloat16
F32 = jnp.float32
M = 128
JW = 16
LV = 128
CZ = 8
ROWS = LV * CZ
PAD = 16
CH = 128
PT = 2 * CH
HALF = ROWS // 2


def iota(shape, dim):
    return lax.broadcasted_iota(jnp.int32, shape, dim)


def pick_rows(idx_ref, scales):
    count = len(scales) * JW
    row, col = iota((count, M), 0), iota((count, M), 1)
    wanted = jnp.zeros((count, M), jnp.int32)
    for j in range(JW):
        wanted = jnp.where(row % JW == j, idx_ref[j], wanted)
    blocks = [
        jnp.where((col == wanted) & (row // JW == d), scale, 0.0).astype(BF)
        for d, scale in enumerate(scales)
    ]
    return jnp.concatenate(blocks, axis=1)


def weighted_columns(sw, first, levels):
    return jnp.concatenate(
        [jnp.broadcast_to(sw[:, y : y + 1], (CZ, M)) for y in range(first, first + levels)], axis=0
    )


def stencil_matrix():
    row, col = iota((PT, PT), 0), iota((PT, PT), 1)
    point = lax.rem(col, CH)
    lev, z = point // CZ, lax.rem(point, CZ)
    up = jnp.where(point + CZ < CH, point + CZ, point + CZ + 16)
    down = jnp.where(point >= CZ, point - CZ, CH + 8 + point)
    ahead = jnp.where(z < CZ - 1, point + 1, CH + 48 + lev)
    behind = jnp.where(z > 0, point - 1, CH + 32 + lev)
    plus = jnp.where(col < CH, up, ahead)
    minus = jnp.where(col < CH, down, behind)
    return (jnp.where(row == plus, 1.0, 0.0) - jnp.where(row == minus, 1.0, 0.0)).astype(BF)


def select_rows():
    row, col = iota((32, CH), 0), iota((32, CH), 1)
    return jnp.where(col == lax.rem(row, 16) * CZ + (row // 16) * (CZ - 1), 1.0, 0.0).astype(BF)


def place():
    gx, gz = lax.axis_index("gx"), lax.axis_index("gz")
    core, zh = lax.rem(gx, 2), gx // 2
    x, low, y = gz // 8, lax.rem(gz // 4, 2), lax.rem(gz, 4)
    return gx, gz, core, x, low, y, x * 4 + y, zh * 2 + low


def plane_peer(p):
    gx, _, _, _, low, _, _, _ = place()
    return (gx, (p // 4) * 8 + low * 4 + lax.rem(p, 4))


def column_peer(p):
    _, _, core, x, _, y, _, _ = place()
    return ((p // 2) * 2 + core, x * 8 + lax.rem(p, 2) * 4 + y)


def reduction_peers():
    _, _, _, _, _, _, q, z = place()
    return [plane_peer(lax.rem(q + d, 16)) for d in range(1, 16)] + [
        column_peer(lax.rem(z + d, 8)) for d in range(1, 8)
    ]


def reduce_parts(
    total, out, part, pair, send, got, column, stack, whole, asend, arecv, bsend, brecv, csend, crecv, dsem
):
    gx, gz, core, x, low, y, q, z = place()
    partner = (gx + 1 - 2 * core, gz)

    width = 8 * M
    own = pl.ds(pl.multiple_of(core * width, width), width)
    theirs = pl.ds(pl.multiple_of((1 - core) * width, width), width)

    def pair_copy(g):
        quarter = pl.ds(g * 4, 4)
        return pltpu.make_async_remote_copy(
            src_ref=part.at[quarter, :, theirs],
            dst_ref=pair.at[quarter],
            send_sem=asend.at[g],
            recv_sem=arecv.at[g],
            device_id=partner,
            device_id_type=MESH,
        )

    def plane_copy(dest, slot):
        return pltpu.make_async_remote_copy(
            src_ref=send.at[dest],
            dst_ref=got.at[slot],
            send_sem=bsend.at[dest],
            recv_sem=brecv.at[slot],
            device_id=plane_peer(dest),
            device_id_type=MESH,
        )

    def column_copy(dest, slot):
        return pltpu.make_async_remote_copy(
            src_ref=column.at[lax.rem(dest, 2)],
            dst_ref=stack.at[slot],
            send_sem=csend.at[dest],
            recv_sem=crecv.at[slot],
            device_id=column_peer(dest),
            device_id_type=MESH,
        )

    for g in range(4):
        for b in range(g * 4, g * 4 + 4):
            for half in range(2):
                owner = (b // 4) * 8 + half * 4 + b % 4
                part[b, half * 4 : half * 4 + 4, :] = total[owner * 4 : owner * 4 + 4, :]
        pair_copy(g).start()
    for g in range(4):
        pair_copy(g).wait_recv()
        for b in range(g * 4, g * 4 + 4):
            send[b] = (part[b, :, own] + pair[b]).astype(BF)

            @pl.when(b != q)
            def _(b=b):
                plane_copy(b, q).start()

    mine = send[q].astype(F32)
    for d in range(1, 16):
        p = lax.rem(q + d, 16)
        plane_copy(p, p).wait_recv()
        mine = mine + got[p].astype(F32)
    column[0] = mine[:4].astype(BF)
    column[1] = mine[4:].astype(BF)
    for d in (4, 3, 5, 2, 6, 1, 7):
        column_copy(lax.rem(z + d, 8), z).start()
    stack[z] = column[low]
    for d in range(1, 8):
        p = lax.rem(z + d, 8)
        column_copy(p, p).wait_recv()
    mine = stack[0].astype(F32)
    for p in range(1, 8):
        mine = mine + stack[p].astype(F32)
    for j in range(8):
        whole[core * 8 + j] = mine[:, j * M : (j + 1) * M]
    block = whole.at[pl.ds(core * 8, 8)]
    last = pltpu.make_async_remote_copy(
        src_ref=block, dst_ref=block, send_sem=dsem.at[0], recv_sem=dsem.at[1],
        device_id=partner, device_id_type=MESH,
    )
    last.start()
    last.wait_recv()
    out[...] = whole[...]

    def finish():
        for g in range(4):
            pair_copy(g).wait_send()
        for d in range(1, 16):
            plane_copy(lax.rem(q + d, 16), q).wait_send()
        for d in range(1, 8):
            column_copy(lax.rem(z + d, 8), z).wait_send()
        last.wait_send()

    return finish


def local_kernel(
    modes, weights, counts, idx, out,
    weights_in, total, planes, near, far, zsend, zgot, sw, swfar, turned, cross_tested, grads, picks, spread, stencil, sel, self_,
    local_sem, near_s, near_r, far_s, far_r, z_s, z_r, w_sem, *reduction,
):
    gx, gz = lax.axis_index("gx"), lax.axis_index("gz")
    odd = lax.rem(gx, 2)
    sign = jnp.where(odd == 0, 0.5, -0.5).astype(F32)
    near_peer = (gx + 1 - 2 * odd, gz)
    far_peer = (lax.rem(gx + 7 + 2 * odd, 8), gz)
    z_peers = ((gx, lax.rem(gz + 31, 32)), (gx, lax.rem(gz + 1, 32)))

    barrier = pltpu.get_barrier_semaphore()
    peers = [near_peer, far_peer, *z_peers, *reduction_peers()]
    small = [pltpu.make_async_copy(weights, weights_in, local_sem.at[6])]
    copies = []
    for c in range(3):
        for side in range(2):
            which = odd if side == 0 else 1 - odd
            copies.append(
                pltpu.make_async_copy(
                    modes.at[c, which], planes.at[c, side, pl.ds(PAD, ROWS)], local_sem.at[2 * c + side]
                )
            )
    for copy in (*small, *copies):
        copy.start()
    for peer in peers:
        pl.semaphore_signal(barrier, inc=1, device_id=peer, device_id_type=MESH)
    for c in range(3):
        for side in range(2):
            planes[c, side, pl.ds(0, PAD), :] = jnp.zeros((PAD, M), BF)
            planes[c, side, pl.ds(PAD + ROWS, PAD), :] = jnp.zeros((PAD, M), BF)
    for copy in small:
        copy.wait()
    for side in range(2):
        which = odd if side == 0 else 1 - odd
        w = weights_in[which]
        sw[side] = jnp.where(iota((CZ, LV), 1) < counts[0], w, jnp.zeros_like(w))
    stencil[...] = stencil_matrix()
    sel[...] = pick_rows(idx, (sign, 0.5, 0.5))
    self_[...] = pick_rows(idx, (sign,))
    ends = select_rows()
    for copy in copies:
        copy.wait()

    def block_of(t):
        return lax.rem(t + 4 * (1 - odd), 8)

    def rows_of(k):
        return pl.ds(pl.multiple_of(PAD + k * CH, 16), CH)

    def near_copy(k):
        return pltpu.make_async_remote_copy(
            src_ref=planes.at[:, 1, rows_of(k)], dst_ref=near.at[k],
            send_sem=near_s.at[k], recv_sem=near_r.at[k], device_id=near_peer, device_id_type=MESH,
        )

    def far_copy(p):
        return pltpu.make_async_remote_copy(
            src_ref=planes.at[:, 0, rows_of(p + 4 * (1 - odd))], dst_ref=far.at[p],
            send_sem=far_s.at[p], recv_sem=far_r.at[p], device_id=far_peer, device_id_type=MESH,
        )

    def z_copy(direction, k):
        return pltpu.make_async_remote_copy(
            src_ref=zsend.at[direction, k], dst_ref=zgot.at[direction, k],
            send_sem=z_s.at[direction, k], recv_sem=z_r.at[direction, k],
            device_id=z_peers[direction], device_id_type=MESH,
        )

    weight_copy = pltpu.make_async_remote_copy(
        src_ref=sw.at[0], dst_ref=swfar, send_sem=w_sem.at[0], recv_sem=w_sem.at[1],
        device_id=far_peer, device_id_type=MESH,
    )

    def send_edges(t, carry):
        k = block_of(t)
        for c in range(3):
            for side in range(2):
                edge = jnp.dot(ends, planes[c, side, rows_of(k), :], preferred_element_type=F32).astype(BF)
                at = (2 * c + side) * 16
                zsend[0, k, at : at + 16, :] = edge[:16]
                zsend[1, k, at : at + 16, :] = edge[16:]
        return carry

    lax.fori_loop(0, 8, send_edges, 0)
    pl.semaphore_wait(barrier, len(peers))
    for t in range(8):
        z_copy(0, block_of(t)).start()
        z_copy(1, block_of(t)).start()
    for p in range(4):
        far_copy(p).start()
    for t in range(8):
        near_copy(lax.rem(t + 4 * odd, 8)).start()
    weight_copy.start()
    for k in range(8):
        for side in range(2):
            wide = weighted_columns(sw[side], k * 16, 16)
            for c in range(3):
                here = planes[c, side, PAD + k * CH : PAD + (k + 1) * CH, :].astype(F32)
                at = c * PT + side * CH
                turned[k, :, at : at + CH] = (here * wide).astype(BF).T

    def prepare(t, b):
        k, with_far = block_of(t), t >= 4
        near_copy(k).wait_recv()
        z_copy(0, k).wait_recv()
        z_copy(1, k).wait_recv()
        if with_far:
            far_copy(t - 4).wait_recv()
        g = grads[b]
        flipped = [[], []]
        for side in range(2):
            lanes = slice(side * CH, (side + 1) * CH)
            for c in range(3):
                at = (2 * c + side) * 16
                stacked = jnp.concatenate(
                    [
                        planes[c, side, rows_of(k), :],
                        planes[c, side, pl.ds(pl.multiple_of(k * CH, 16), 16), :],
                        planes[c, side, pl.ds(pl.multiple_of(PAD + (k + 1) * CH, 16), 16), :],
                        zgot[1, k, at : at + 16, :],
                        zgot[0, k, at : at + 16, :],
                        jnp.zeros((64, M), BF),
                    ],
                    axis=0,
                ).T
                both = jnp.dot(stacked, stencil[...], preferred_element_type=F32)
                g[3 + c, :, lanes] = both[:, :CH]
                g[6 + c, :, lanes] = both[:, CH:]
                flipped[side].append(stacked[:, :CH])
            pk = jnp.dot(sel[...], jnp.concatenate(flipped[side], axis=0), preferred_element_type=F32)
            for r in range(3 * JW):
                picks[b][r, :, lanes] = jnp.broadcast_to(pk[r : r + 1], (8, CH))
        for c in range(3):
            inner = flipped[1][c].astype(F32)
            if with_far:
                inner = inner - far[t - 4, c].T.astype(F32)
            g[c, :, :CH] = inner
            g[c, :, CH:] = near[k, c].T.astype(F32) - flipped[0][c].astype(F32)

    def terms(b, step, target):
        g, pk = grads[b], picks[b]
        scale = []
        for h in range(2):
            p = [pk[d * JW + 2 * step + h] for d in range(3)]
            scale.append([jnp.concatenate([v, v], axis=0) for v in p])
        for c in range(3):
            for u in range(8):
                tile = slice(u * 16, u * 16 + 16)
                gx_, gy_, gz_ = g[c, tile, :], g[3 + c, tile, :], g[6 + c, tile, :]
                for h in range(2):
                    px, py, pz = scale[h]
                    value = px * gx_ + py * gy_ + pz * gz_
                    target[h * M + u * 16 : h * M + u * 16 + 16, c * PT : (c + 1) * PT] = value.astype(BF)

    def prepare_cross(v, b):
        if v == 0:
            weight_copy.wait_recv()
        foreign = swfar[...]
        foreign = jnp.where(odd == 1, pltpu.roll(foreign, LV // 2, 1), foreign)
        wide = [weighted_columns(foreign, v * 32 + 16 * h, 16) for h in range(2)]
        pk = []
        for h in range(2):
            mine = 2 * v + h + 4 * odd
            for c in range(3):
                here = far[2 * v + h, c]
                if c == 0:
                    pk.append(jnp.dot(self_[...], here.T, preferred_element_type=F32).astype(BF))
                at = c * PT + h * CH
                cross_tested[v, :, at : at + CH] = (here.astype(F32) * wide[h]).astype(BF).T
                grads[b][c, :, h * CH : (h + 1) * CH] = planes[c, 0, rows_of(mine), :].T.astype(F32)
            for j in range(JW):
                picks[b][j, :, h * CH : (h + 1) * CH] = jnp.broadcast_to(
                    pk[h][j : j + 1].astype(F32), (8, CH)
                )

    def cross_terms(b, step, target):
        scale = []
        for h in range(2):
            p = picks[b][2 * step + h].astype(BF)
            scale.append(jnp.concatenate([p, p], axis=0))
        for c in range(3):
            for u in range(8):
                tile = grads[b][c, u * 16 : u * 16 + 16, :].astype(BF)
                for h in range(2):
                    target[h * M + u * 16 : h * M + u * 16 + 16, c * PT : (c + 1) * PT] = scale[h] * tile

    stages = []
    for kind, n in [(0, t) for t in range(6)] + [(1, 0), (0, 6), (0, 7), (1, 1)]:
        b = len(stages) % 2
        if kind == 0:
            made, form = functools.partial(prepare, n, b), functools.partial(terms, b)
            stages.append((made, form, lambda n=n: turned[block_of(n)]))
        else:
            made, form = functools.partial(prepare_cross, n, b), functools.partial(cross_terms, b)
            stages.append((made, form, lambda n=n: cross_tested[n]))
    waiting = None
    stages[0][0]()
    for i, (_, form, tested) in enumerate(stages):
        for step in range(8):
            if waiting is not None:
                waiting()

            def waiting(step=step, tested=tested, fresh=i == 0):
                value = lax.dot_general(
                    tested(),
                    spread[step % 4][...],
                    (((1,), (1,)), ((), ())),
                    preferred_element_type=F32,
                )
                cols = slice(step * 256, step * 256 + 256)
                total[:, cols] = value if fresh else total[:, cols] + value

            form(step, spread[step % 4])
            if step == 5 and i + 1 < len(stages):
                stages[i + 1][0]()
    waiting()

    finish = reduce_parts(total, out, *reduction)
    for k in range(8):
        near_copy(k).wait_send()
        z_copy(0, k).wait_send()
        z_copy(1, k).wait_send()
        if k < 4:
            far_copy(k).wait_send()
    weight_copy.wait_send()
    finish()


VM = pl.BlockSpec(memory_space=pltpu.VMEM)
SM = pl.BlockSpec(memory_space=pltpu.SMEM)
HB = pl.BlockSpec(memory_space=pl.ANY)


def local(modes, weights, counts, mode_index):
    return pl.pallas_call(
        local_kernel,
        out_shape=jax.ShapeDtypeStruct((JW, 4, M), F32),
        in_specs=[HB, HB, SM, SM],
        out_specs=VM,
        scratch_shapes=[
            pltpu.VMEM((2, CZ, LV), F32),
            pltpu.VMEM((M, JW * M), F32),
            pltpu.VMEM((3, 2, ROWS + 2 * PAD, M), BF),
            pltpu.VMEM((8, 3, CH, M), BF),
            pltpu.VMEM((4, 3, CH, M), BF),
            pltpu.VMEM((2, 8, 96, M), BF),
            pltpu.VMEM((2, 8, 96, M), BF),
            pltpu.VMEM((2, CZ, LV), F32),
            pltpu.VMEM((CZ, LV), F32),
            pltpu.VMEM((8, M, 3 * PT), BF),
            pltpu.VMEM((2, M, 3 * PT), BF),
            [pltpu.VMEM((9, M, PT), F32)] * 2,
            [pltpu.VMEM((3 * JW, 8, PT), F32)] * 2,
            [pltpu.VMEM((2 * M, 3 * PT), BF)] * 4,
            pltpu.VMEM((PT, PT), BF),
            pltpu.VMEM((3 * JW, 3 * M), BF),
            pltpu.VMEM((JW, M), BF),
            pltpu.SemaphoreType.DMA((7,)),
            pltpu.SemaphoreType.DMA((8,)),
            pltpu.SemaphoreType.DMA((8,)),
            pltpu.SemaphoreType.DMA((4,)),
            pltpu.SemaphoreType.DMA((4,)),
            pltpu.SemaphoreType.DMA((2, 8)),
            pltpu.SemaphoreType.DMA((2, 8)),
            pltpu.SemaphoreType.DMA((2,)),
            pltpu.VMEM((16, 8, JW * M), F32),
            pltpu.VMEM((16, 8, 8 * M), F32),
            pltpu.VMEM((16, 8, 8 * M), BF),
            pltpu.VMEM((16, 8, 8 * M), BF),
            pltpu.VMEM((2, 4, 8 * M), BF),
            pltpu.VMEM((8, 4, 8 * M), BF),
            pltpu.VMEM((JW, 4, M), F32),
            pltpu.SemaphoreType.DMA((4,)),
            pltpu.SemaphoreType.DMA((4,)),
            pltpu.SemaphoreType.DMA((16,)),
            pltpu.SemaphoreType.DMA((16,)),
            pltpu.SemaphoreType.DMA((8,)),
            pltpu.SemaphoreType.DMA((8,)),
            pltpu.SemaphoreType.DMA((2,)),
        ],
        compiler_params=pltpu.CompilerParams(
            vmem_limit_bytes=67043328, collective_id=0, has_side_effects=True
        ),
    )(modes.reshape(3, 2, ROWS, M), jnp.swapaxes(weights, 1, 2), counts, mode_index)


def solution(mesh):
    placed = (P(None, "gx", None, "gz", None), P("gx", None, "gz"), P(("gx", "gz")), P())
    return jax.shard_map(
        local, mesh=mesh, in_specs=placed, out_specs=P(None, "gz", None), check_vma=False
    )
```
